32 devices in a mesh: seq: 16 (over z, y, x), mp: 2 (over core).
Axes of the slice: x: 2, y: 2, z: 4, core: 2. Of those that a mesh axis runs over, the one named last changes fastest.
Arguments:
- states: bfloat16 [4096, 768], P('seq'), may hold values from -24 to 24
- qkv_weight: bfloat16 [3, 768, 768], P(None, None, 'mp'), may hold values from -0.21875 to 0.21875
- out_weight: bfloat16 [768, 768], P('mp'), may hold values from -0.21875 to 0.21875
- up_weight: bfloat16 [768, 3072], P(None, 'mp'), may hold values from -0.21875 to 0.21875
- down_weight: bfloat16 [3072, 768], P('mp'), may hold values from -0.109375 to 0.109375
- attn_gain: float32 [768], replicated, may hold values from 0.5 to 1.5
- mlp_gain: float32 [768], replicated, may hold values from 0.5 to 1.5
- global_ids: int32 [2], replicated, may hold values from 0 to 63, as said below
- random_owner: int32 [2, 64, 6, 3], P('mp', 'seq'), may hold values from 0 to 15, all different within a row; in each aligned block of 24 rows (0 to 23, 24 to 47, ..., all dimensions but the last counted through in order) at most 5 rows name the same one
- random_local: int32 [2, 64, 6, 3], P('mp', 'seq'), may hold values from 0 to 3
Outputs:
- layer_out: bfloat16 [4096, 768], P('seq')
The draws below stay inside these ranges and needn't reach their ends.
Inputs may be any that keep to these rules, and one draw needn't show every extreme that they name: `global_ids`: 2 different block numbers; the second is 63. The random key block is random_owner * 4 + random_local. For one query block and head the 3 owners differ. Within the rows of one device (aligned blocks of 4 * K rows over the first three dimensions, K the third dimension) no owner is named more than 5 times, a bound that some block reaches.
All inputs are finite; a program needn't handle non-finite values.
Results may differ from the reference program's by a relative error of at most 0.008.
The reference program's roundings to bfloat16 on the way count: a program that leaves them out, or rounds other values in their place, can miss the bound.
Values may be sent and summed in bfloat16 or wider, within the bound.
A program may use at most 192 MiB of HBM per device.

```python
import math
import jax
import jax.numpy as jnp
import numpy as np
from jax import lax

D = 768
H = 12
HD = 64
FF = 3072
BS = 64
R = 3
G = 2
QB_DEV = 4
TOKENS = 4096
NB = 64
MOST = 5
N_SEQ = 16
N_MP = 2


def chosen_blocks(key):
    first = jax.random.randint(jax.random.fold_in(key, 11), (1,), 0, NB - 1)
    return jnp.concatenate([first, jnp.full((1,), NB - 1)]).astype(jnp.int32)


def draw_global_ids(key, part):
    return chosen_blocks(key)


def draw_states(key, part):
    split_keys = jax.random.split(jax.random.fold_in(key, 23), 5)
    starts = chosen_blocks(key) * BS + 3
    picked = jax.random.randint(split_keys[3], (8,), BS // 2, TOKENS - BS)
    anchors = jnp.concatenate([starts, picked])
    direction = jax.random.uniform(split_keys[2], (D,), jnp.float32, -1.7, 1.7)
    jitter = jax.random.normal(split_keys[4], (2, anchors.shape[0], D), jnp.float32) * 0.05
    sample = jax.random.normal(split_keys[1], (TOKENS, D), jnp.float32)
    strength = jnp.linspace(2.5, 3.5, anchors.shape[0]).astype(jnp.float32)
    first_rows = strength[:, None] * direction[None, :] + jitter[0]
    second_rows = strength[:, None] * direction[None, :] * 1.01 + jitter[1]
    sample = sample.at[anchors].set(first_rows).at[anchors + 1].set(second_rows)
    return jnp.clip(sample, -6.0, 6.0).astype(jnp.bfloat16)


def place_ends(array, rng, low, largest):
    place = [jax.random.randint(jax.random.fold_in(rng, axis), (), 0, length) for axis, length in enumerate(array.shape)]
    longest = array.shape.index(max(array.shape))
    neighbour = place[:longest] + [(place[longest] + 1) % array.shape[longest]] + place[longest + 1:]
    return array.at[tuple(place)].set(low).at[tuple(neighbour)].set(largest)


def levels(key, extent, shards, low, high):
    loudness, own = 1.0, jax.random.fold_in(key, 6)
    for dim, shards_of in shards:
        steps = jnp.exp(jax.random.uniform(jax.random.fold_in(own, dim), (shards_of,), jnp.float32, low / len(shards), high / len(shards)))
        loudness = loudness * jnp.repeat(steps, extent[dim] // shards_of).reshape([-1 if axis == dim else 1 for axis in range(len(extent))])
    return loudness


def shared_out(stream_key, own, number, rows, count, top, most, lean):
    ranking = jax.random.permutation(stream_key, count)
    crowded, usual = shares(count, rows * top, most, lean, True), shares(count, rows * top, most, lean, False)
    places = jnp.arange(count)

    def named(tallies, rotation):
        used = int((tallies > 0).sum())
        fixed = max(1, used // 4)
        moved = fixed + (places - fixed + rotation * (used - fixed)) % max(1, count - fixed)
        return jnp.zeros((count,), jnp.int32).at[ranking[jnp.where(places < fixed, places, moved)]].set(jnp.asarray(tallies, jnp.int32))

    tallies = jnp.where(number % 4 == 0, named(crowded, number // 4), named(usual, number - number // 4 - 1))
    mixed = jax.random.permutation(jax.random.fold_in(own, 3), count)
    donor, sink = mixed[0:count // 2 * 2:2], mixed[1:count // 2 * 2:2]
    room = jnp.minimum(tallies[donor] - 1, most - tallies[sink]) // 2
    room = jnp.where((donor == ranking[0]) | (sink == ranking[0]) | (tallies[sink] == 0), 0, jnp.maximum(room, 0))
    moved = jax.random.randint(jax.random.fold_in(own, 4), (count // 2,), 0, 1 << 20) % (room + 1)
    tallies = tallies.at[donor].add(-moved).at[sink].add(moved)
    items = jnp.searchsorted(jnp.cumsum(tallies), jnp.arange(rows * top), side="right").astype(jnp.int32)
    grid = items.reshape(top, rows).T
    grid = grid[jax.random.permutation(jax.random.fold_in(own, 1), rows)]
    rotation = jax.random.randint(jax.random.fold_in(own, 2), (rows, 1), 0, top)
    return jnp.take_along_axis(grid, (jnp.arange(top)[None, :] + rotation) % top, axis=1)


def shares(number_of, total, reach, skew, full):
    weights = [(1 << 20) // math.isqrt(rank ** skew) + 1 for rank in range(1, number_of + 1)]
    largest = reach if full else min(reach, max(-(-total // number_of), total * weights[0] // sum(weights)))
    least = 1 if total - largest >= number_of - 1 else 0
    holding, spare = [largest] + [least] * (number_of - 1), total - largest - least * (number_of - 1)
    while spare > 0:
        free = [i for i in range(1, number_of) if holding[i] < largest] or [i for i in range(1, number_of) if holding[i] < reach]
        mass, left = sum([weights[i] for i in free]), spare
        for i in free:
            addition = min(reach - holding[i], max(1, left * weights[i] // mass), spare)
            holding[i] = holding[i] + addition
            spare = spare - addition
    return np.array(holding)


def noise(own_key, extent, scale, bound, pieces=(), held_as=jnp.bfloat16):
    array = scale * jax.random.normal(own_key, extent, jnp.float32)
    if pieces:
        array = array * levels(own_key, extent, pieces, -0.22, 0.18)
    return jnp.clip(array, -bound, bound).astype(held_as)


def setup_inputs(seed: int = 0) -> dict:
    seeds = jax.random.split(jax.random.key(seed), 11)
    states = draw_states(jax.random.fold_in(seeds[10], 71), 0)
    qkv_weight = noise(seeds[1], (3, D, D), D ** -0.5, 0.21875, ((2, 2),))
    out_weight = noise(seeds[2], (D, D), D ** -0.5, 0.21875, ((0, 2),))
    up_weight = noise(seeds[3], (D, FF), D ** -0.5, 0.21875, ((1, 2),))
    down_weight = noise(seeds[4], (FF, D), FF ** -0.5, 0.109375, ((0, 2),))
    attn_gain = jnp.clip(1.0 + 0.1 * jax.random.normal(seeds[5], (D,), jnp.float32), 0.5, 1.5)
    mlp_gain = jnp.clip(1.0 + 0.1 * jax.random.normal(seeds[6], (D,), jnp.float32), 0.5, 1.5)
    global_ids = draw_global_ids(jax.random.fold_in(seeds[10], 71), 0)
    random_owner_keys = jax.random.split(jax.random.fold_in(seeds[8], 1), N_MP * NB * (H // N_MP) // (QB_DEV * (H // N_MP)))
    random_owner_turns = jax.random.permutation(jax.random.fold_in(seeds[8], 3), N_MP * NB * (H // N_MP) // (QB_DEV * (H // N_MP)))
    random_owner = jax.vmap(lambda own, number: shared_out(jax.random.fold_in(seeds[8], 2), own, number, QB_DEV * (H // N_MP), N_SEQ, R, MOST, 2))(random_owner_keys, random_owner_turns).reshape((N_MP, NB, H // N_MP, R))
    random_local = place_ends(jax.random.randint(seeds[9], (N_MP, NB, H // N_MP, R), 0, QB_DEV), jax.random.fold_in(seeds[9], 1), 0, QB_DEV - 1).astype(jnp.int32)
    return dict(states=states, qkv_weight=qkv_weight, out_weight=out_weight, up_weight=up_weight, down_weight=down_weight, attn_gain=attn_gain, mlp_gain=mlp_gain, global_ids=global_ids, random_owner=random_owner, random_local=random_local)


EPSILON = 1e-05
NEGATIVE = -1e+30

def layer_norm(inputs, scales):
    center = lax.optimization_barrier(jnp.mean(inputs, axis=-1, keepdims=True))
    shifted = inputs - center
    spread = lax.optimization_barrier(jnp.mean(shifted * shifted, axis=-1, keepdims=True))
    return shifted * lax.rsqrt(spread + EPSILON) * scales.astype(jnp.float32)

def softmax_rows(scores):
    highest = lax.optimization_barrier(jnp.max(scores, axis=-1, keepdims=True))
    raised = jnp.exp(scores - highest)
    return raised / lax.optimization_barrier(jnp.sum(raised, axis=-1, keepdims=True))

def reference(states, qkv_weight, out_weight, up_weight, down_weight, attn_gain, mlp_gain, global_ids, random_owner, random_local):
    block_count = TOKENS // BS
    scaling = HD ** (-0.5)
    highest = lax.Precision.HIGHEST
    query_all = jnp.dot(states, qkv_weight[0], preferred_element_type=jnp.float32).astype(jnp.bfloat16)
    key_all = jnp.dot(states, qkv_weight[1], preferred_element_type=jnp.float32).astype(jnp.bfloat16)
    value_all = jnp.dot(states, qkv_weight[2], preferred_element_type=jnp.float32).astype(jnp.bfloat16)
    query_heads = query_all.reshape(block_count, BS, H, HD)
    key_heads = key_all.reshape(block_count, BS, H, HD).transpose(0, 2, 1, 3)
    value_heads = value_all.reshape(block_count, BS, H, HD).transpose(0, 2, 1, 3)
    random_ids = (random_owner * QB_DEV + random_local).transpose(1, 0, 2, 3).reshape(block_count, H, R)
    head_range = jnp.arange(H, dtype=jnp.int32)
    global_keys = key_heads[global_ids].astype(jnp.float32)
    global_values = value_heads[global_ids].astype(jnp.float32)

    def sparse_group(first_block):
        block_ids = first_block + jnp.arange(QB_DEV, dtype=jnp.int32)
        query_part = lax.dynamic_slice_in_dim(query_heads, first_block, QB_DEV, 0).astype(jnp.float32)
        offsets = block_ids[:, None] + jnp.arange(-1, 2, dtype=jnp.int32)[None, :]
        inside = (offsets >= 0) & (offsets < block_count)
        clipped = jnp.clip(offsets, 0, block_count - 1)
        window_keys = key_heads[clipped].astype(jnp.float32)
        window_values = value_heads[clipped].astype(jnp.float32)
        chosen = random_ids[block_ids]
        random_keys = key_heads[chosen, head_range[None, :, None]].astype(jnp.float32)
        random_values = value_heads[chosen, head_range[None, :, None]].astype(jnp.float32)
        score_window = jnp.einsum('bqhd,bwhkd->bhqwk', query_part, window_keys, precision=highest) * scaling
        score_window = jnp.where(inside[:, None, None, :, None], score_window, NEGATIVE)
        score_random = jnp.einsum('bqhd,bhrkd->bhqrk', query_part, random_keys, precision=highest) * scaling
        score_global = jnp.einsum('bqhd,ghkd->bhqgk', query_part, global_keys, precision=highest) * scaling
        joined = jnp.concatenate([score_window, score_random, score_global], axis=3)
        joined_shape = joined.shape
        flat_weights = softmax_rows(joined.reshape(joined_shape[0], joined_shape[1], joined_shape[2], -1))
        weights = lax.optimization_barrier(flat_weights.astype(jnp.bfloat16)).astype(jnp.float32).reshape(joined_shape)
        result = jnp.einsum('bhqwk,bwhkd->bqhd', weights[:, :, :, :3], window_values, precision=highest)
        result = result + jnp.einsum('bhqrk,bhrkd->bqhd', weights[:, :, :, 3:3 + R], random_values, precision=highest)
        result = result + jnp.einsum('bhqgk,ghkd->bqhd', weights[:, :, :, 3 + R:], global_values, precision=highest)
        return result
    sparse = lax.map(sparse_group, jnp.arange(N_SEQ, dtype=jnp.int32) * QB_DEV)
    sparse = sparse.reshape(block_count, BS, H, HD)
    global_queries = query_heads[global_ids].astype(jnp.float32).transpose(2, 0, 1, 3).reshape(H, G * BS, HD)
    every_key = key_heads.transpose(1, 0, 2, 3).reshape(H, TOKENS, HD)
    every_value = value_heads.transpose(1, 0, 2, 3).reshape(H, TOKENS, HD)

    def global_head(inputs):
        query_rows, key_rows, value_rows = inputs
        scores = jnp.dot(query_rows, key_rows.astype(jnp.float32).T, precision=highest) * scaling
        return jnp.dot(softmax_rows(scores), value_rows.astype(jnp.float32), precision=highest)
    global_out = lax.map(global_head, (global_queries, every_key, every_value))
    global_out = global_out.reshape(H, G, BS, HD).transpose(1, 2, 0, 3)
    sparse = sparse.at[global_ids].set(global_out)
    attended = sparse.astype(jnp.bfloat16).reshape(TOKENS, D)
    projected = jnp.dot(attended, out_weight, preferred_element_type=jnp.float32)
    normed = layer_norm(states.astype(jnp.float32) + projected, attn_gain).astype(jnp.bfloat16)
    hidden = jax.nn.gelu(jnp.dot(normed, up_weight, preferred_element_type=jnp.float32), approximate=False).astype(jnp.bfloat16)
    expanded = jnp.dot(hidden, down_weight, preferred_element_type=jnp.float32)
    return layer_norm(normed.astype(jnp.float32) + expanded, mlp_gain).astype(jnp.bfloat16)
```

```python
import functools

import jax
import jax.numpy as jnp
from jax import lax
from jax.experimental import pallas as pl
from jax.experimental.pallas import tpu as pltpu
from jax.sharding import PartitionSpec as P

HD = 64
BS = 64
R = 3
LANES = 128
MESH = pl.DeviceIdType.MESH

EPSILON = 1e-05
NEGATIVE = -1e30


def layer_norm(inputs, scales):
    center = jnp.mean(inputs, axis=-1, keepdims=True)
    shifted = inputs - center
    spread = jnp.mean(shifted * shifted, axis=-1, keepdims=True)
    return shifted * lax.rsqrt(spread + EPSILON) * scales


def dot_t(a, b):
    return lax.dot_general(a, b, (((1,), (1,)), ((), ())), preferred_element_type=jnp.float32)


def dot(a, b):
    return jnp.dot(a, b, preferred_element_type=jnp.float32)


def swap_halves(x):
    return pltpu.roll(x, HD, 1)


def attend_kernel(
    n,
    cap,
    heads,
    blocks,
    g_count,
    states,
    weight,
    wanted,
    slot,
    gids,
    att,
    tab,
    tab_s,
    cand,
    cand_in,
    pick,
    gath,
    gstates,
    kvb,
    qpad,
    stage,
    rr,
    halo_l,
    halo_r,
    win,
    gq,
    gkv,
    part,
    part_in,
    gmine,
    gout,
    s_tab,
    r_tab,
    s_cand,
    r_cand,
    s_gath,
    r_gath,
    s_rand,
    r_rand,
    s_halo,
    r_halo,
    s_part,
    r_part,
    s_gout,
    r_gout,
    l_sem,
):
    me = lax.axis_index("seq")
    pairs = heads // 2
    width = states.shape[1]
    cols = width // LANES
    quarters = BS // 16
    units = g_count * cols * quarters
    per = cand_in.shape[1]
    cand_parts = units // per
    rows_per = part_in.shape[1]
    part_parts = part.shape[0] // rows_per
    left = lax.rem(me + n - 1, n)
    right = lax.rem(me + 1, n)

    def peer(k):
        return lax.rem(me + k, n)

    def each_peer(body):
        def step(k, carry):
            body(peer(k))
            return carry

        lax.fori_loop(1, n, step, 0)

    def guarded(limit, who, body):
        if limit < n:
            pl.when(who < limit)(body)
        else:
            body()

    def remote(src, dst, ssem, rsem, d):
        return pltpu.make_async_remote_copy(
            src_ref=src,
            dst_ref=dst,
            send_sem=ssem,
            recv_sem=rsem,
            device_id={"seq": d},
            device_id_type=MESH,
        )

    def tab_copy(d, owner):
        return remote(wanted.at[d], tab.at[owner], s_tab.at[d], r_tab.at[owner], d)

    def cand_copy(d, owner):
        return remote(
            cand.at[pl.ds(d * per, per)], cand_in.at[owner], s_cand.at[d], r_cand.at[owner], d
        )

    def gath_copy(d, owner):
        return remote(
            pick, gath.at[pl.ds(owner * per, per)], s_gath.at[d], r_gath.at[owner], d
        )

    def rand_copy(d, owner):
        return remote(
            stage.at[pl.ds(d * cap, cap)],
            rr.at[pl.ds(owner * cap, cap)],
            s_rand.at[d],
            r_rand.at[owner],
            d,
        )

    def part_copy(d, owner):
        return remote(
            part.at[pl.ds(pl.multiple_of(d * rows_per, 8), rows_per)],
            part_in.at[owner],
            s_part.at[d],
            r_part.at[owner],
            d,
        )

    def gout_copy(d, owner):
        return remote(
            gmine,
            gout.at[pl.ds(pl.multiple_of(owner * rows_per, 8), rows_per)],
            s_gout.at[d],
            r_gout.at[owner],
            d,
        )

    to_right = remote(
        kvb.at[pl.ds((blocks - 1) * heads, heads)], halo_l, s_halo.at[0], r_halo.at[0], right
    )
    to_left = remote(kvb.at[pl.ds(0, heads)], halo_r, s_halo.at[1], r_halo.at[1], left)

    for g in range(g_count):
        local = lax.rem(gids[g], blocks)
        for j in range(cols):
            cut = slice(j * LANES, (j + 1) * LANES)
            piece = states[0:BS, cut]
            for b in range(1, blocks):
                piece = jnp.where(local == b, states[b * BS : (b + 1) * BS, cut], piece)
            for q in range(quarters):
                cand[(g * cols + j) * quarters + q] = piece[q * 16 : (q + 1) * 16]

    barrier = pltpu.get_barrier_semaphore()
    each_peer(
        lambda d: pl.semaphore_signal(barrier, inc=1, device_id={"seq": d}, device_id_type=MESH)
    )
    pl.semaphore_wait(barrier, n - 1)

    each_peer(lambda d: tab_copy(d, me).start())
    each_peer(lambda d: guarded(cand_parts, d, lambda: cand_copy(d, me).start()))
    tab[me] = wanted[me]

    def own_cand():
        cand_in[me] = cand[pl.ds(me * per, per)]

    guarded(cand_parts, me, own_cand)

    lane = lax.broadcasted_iota(jnp.int32, (BS, LANES), 1)
    low = lane < HD
    x = states[...]
    for j in range(pairs):
        cut = slice(j * LANES, (j + 1) * LANES)
        k = dot(x, weight[1, :, cut])
        v = dot(x, weight[2, :, cut])
        for b in range(blocks):
            kb, vb = k[b * BS : (b + 1) * BS], v[b * BS : (b + 1) * BS]
            kvb[b * heads + 2 * j] = jnp.where(low, kb, swap_halves(vb)).astype(jnp.bfloat16)
            kvb[b * heads + 2 * j + 1] = jnp.where(low, swap_halves(kb), vb).astype(jnp.bfloat16)

    to_right.start()
    to_left.start()

    each_peer(lambda d: tab_copy(d, d).wait_recv())
    table = pltpu.make_async_copy(tab, tab_s, l_sem)
    table.start()
    table.wait()

    def serve(d):
        for c in range(cap):
            stage[d * cap + c] = kvb[tab_s[d, 0, c]]
        rand_copy(d, me).start()

    each_peer(serve)
    for c in range(cap):
        rr[me * cap + c] = kvb[tab_s[me, 0, c]]

    def relay():
        each_peer(lambda d: cand_copy(d, d).wait_recv())
        for u in range(per):
            g = (me * per + u) // (cols * quarters)
            wanted_id = gids[g]

            def choose(d, so_far):
                here = (wanted_id >= d * blocks) & (wanted_id < (d + 1) * blocks)
                return jnp.where(here, cand_in[d, u], so_far)

            pick[u] = lax.fori_loop(1, n, choose, cand_in[0, u])
        gath[pl.ds(me * per, per)] = pick[...]
        each_peer(lambda d: gath_copy(d, me).start())

    guarded(cand_parts, me, relay)

    scaling = HD ** (-0.5)
    for j in range(pairs):
        cut = slice(j * LANES, (j + 1) * LANES)
        q = dot(x, weight[0, :, cut]).astype(jnp.bfloat16).astype(jnp.float32) * scaling
        for b in range(blocks):
            qb = q[b * BS : (b + 1) * BS]
            qpad[b * heads + 2 * j] = jnp.where(low, qb, 0.0).astype(jnp.bfloat16)
            qpad[b * heads + 2 * j + 1] = jnp.where(low, swap_halves(qb), 0.0).astype(jnp.bfloat16)

    each_peer(lambda d: guarded(cand_parts, d, lambda: gath_copy(d, d).wait_recv()))
    for g in range(g_count):
        for j in range(cols):
            for q in range(quarters):
                gstates[g * BS + q * 16 : g * BS + (q + 1) * 16, j * LANES : (j + 1) * LANES] = (
                    gath[(g * cols + j) * quarters + q]
                )
    gx = gstates[...]
    rows = g_count * BS
    glane = lax.broadcasted_iota(jnp.int32, (rows, LANES), 1)
    glow = glane < HD
    for j in range(pairs):
        cut = slice(j * LANES, (j + 1) * LANES)
        q = dot(gx, weight[0, :, cut]).astype(jnp.bfloat16).astype(jnp.float32) * scaling
        k = dot(gx, weight[1, :, cut])
        v = dot(gx, weight[2, :, cut])
        gq[2 * j] = jnp.where(glow, q, 0.0).astype(jnp.bfloat16)
        gq[2 * j + 1] = jnp.where(glow, swap_halves(q), 0.0).astype(jnp.bfloat16)
        gkv[2 * j] = jnp.where(glow, k, swap_halves(v)).astype(jnp.bfloat16)
        gkv[2 * j + 1] = jnp.where(glow, swap_halves(k), v).astype(jnp.bfloat16)

    for h in range(heads):
        keys = jnp.concatenate([kvb[b * heads + h] for b in range(blocks)], axis=0)
        s = dot_t(gq[h], keys)
        high = jnp.max(s, axis=-1, keepdims=True)
        e = jnp.exp(s - high)
        total = jnp.sum(e, axis=-1, keepdims=True)
        e_high = e.astype(jnp.bfloat16)
        e_low = (e - e_high.astype(jnp.float32)).astype(jnp.bfloat16)
        acc = dot(e_high, keys) + dot(e_low, keys)
        part[h * rows : (h + 1) * rows] = jnp.where(
            glane < HD // 2, high, jnp.where(glow, total, acc)
        )
    each_peer(lambda d: guarded(part_parts, d, lambda: part_copy(d, me).start()))

    to_right.wait_recv()
    to_left.wait_recv()
    win[0:heads] = halo_l[...]
    win[heads : heads + blocks * heads] = kvb[...]
    win[heads + blocks * heads :] = halo_r[...]

    def combine():
        part_in[me] = part[pl.ds(pl.multiple_of(me * rows_per, 8), rows_per)]
        each_peer(lambda d: part_copy(d, d).wait_recv())

        def top(d, best):
            return jnp.maximum(best, part_in[d])

        best = lax.fori_loop(1, n, top, part_in[0])[:, 0:1]

        def add(d, so_far):
            piece = part_in[d]
            return so_far + piece * jnp.exp(piece[:, 0:1] - best)

        summed = lax.fori_loop(0, n, add, jnp.zeros((rows_per, LANES), jnp.float32))
        done = summed / summed[:, HD // 2 : HD // 2 + 1]
        gmine[...] = done
        gout[pl.ds(pl.multiple_of(me * rows_per, 8), rows_per)] = done
        each_peer(lambda d: gout_copy(d, me).start())

    guarded(part_parts, me, combine)

    each_peer(lambda d: rand_copy(d, d).wait_recv())

    slots = 3 + R + g_count
    slot_lane = lax.broadcasted_iota(jnp.int32, (BS, slots * BS), 1)

    def block_step(b, carry):
        first = me * blocks + b
        start = jnp.where(first == 0, BS, 0)
        stop = jnp.where(first == n * blocks - 1, 2 * BS, 3 * BS)
        outside = (slot_lane < start) | ((slot_lane >= stop) & (slot_lane < 3 * BS))
        for j in range(pairs):
            halves = []
            for h in (2 * j, 2 * j + 1):
                at = b * heads + h
                keys = jnp.concatenate(
                    [win[at + t * heads] for t in range(3)]
                    + [rr[slot[at * R + r]] for r in range(R)]
                    + [gkv[h]],
                    axis=0,
                )
                s = jnp.where(outside, NEGATIVE, dot_t(qpad[at], keys))
                e = jnp.exp(s - jnp.max(s, axis=-1, keepdims=True))
                w = (e * (1.0 / jnp.sum(e, axis=-1, keepdims=True))).astype(jnp.bfloat16)
                halves.append(dot(w, keys))
            att[j, pl.ds(pl.multiple_of(b * BS, BS), BS), :] = jnp.where(
                low, swap_halves(halves[0]), halves[1]
            ).astype(jnp.bfloat16)
        return carry

    lax.fori_loop(0, blocks, block_step, 0)

    each_peer(lambda d: guarded(part_parts, d, lambda: gout_copy(d, d).wait_recv()))
    for j in range(pairs):
        for g in range(g_count):
            lo = (2 * j * g_count + g) * BS
            hi = ((2 * j + 1) * g_count + g) * BS
            row = jnp.where(low, swap_halves(gout[lo : lo + BS]), gout[hi : hi + BS])
            row = row.astype(jnp.bfloat16).astype(jnp.float32)
            for b in range(blocks):
                here = gids[g] == me * blocks + b
                old = att[j, b * BS : (b + 1) * BS, :].astype(jnp.float32)
                att[j, b * BS : (b + 1) * BS, :] = jnp.where(here, row, old).astype(jnp.bfloat16)

    def drain(d):
        tab_copy(d, me).wait_send()
        guarded(cand_parts, d, lambda: cand_copy(d, me).wait_send())
        guarded(cand_parts, me, lambda: gath_copy(d, me).wait_send())
        rand_copy(d, me).wait_send()
        guarded(part_parts, d, lambda: part_copy(d, me).wait_send())
        guarded(part_parts, me, lambda: gout_copy(d, me).wait_send())

    each_peer(drain)
    to_right.wait_send()
    to_left.wait_send()


def tail_kernel(
    chunks,
    att,
    states,
    out_w,
    up_w,
    down_w,
    gain1,
    gain2,
    out,
    mine1,
    theirs1,
    mine2,
    theirs2,
    s1,
    r1,
    s2,
    r2,
    normed,
):
    other = 1 - lax.axis_index("mp")
    barrier = pltpu.get_barrier_semaphore()
    pl.semaphore_signal(barrier, inc=1, device_id={"mp": other}, device_id_type=MESH)
    pl.semaphore_wait(barrier, 1)
    rows = states.shape[0] // chunks

    def swap(mine, theirs, ssem, rsem, c):
        return pltpu.make_async_remote_copy(
            src_ref=mine.at[c],
            dst_ref=theirs.at[c],
            send_sem=ssem.at[c],
            recv_sem=rsem.at[c],
            device_id={"mp": other},
            device_id_type=MESH,
        )

    for c in range(chunks):
        cut = slice(c * rows, (c + 1) * rows)
        acc = dot(att[0, cut, :], out_w[0:LANES, :])
        for j in range(1, att.shape[0]):
            acc = acc + dot(att[j, cut, :], out_w[j * LANES : (j + 1) * LANES, :])
        mine1[c] = acc.astype(mine1.dtype)
        swap(mine1, theirs1, s1, r1, c).start()
    for c in range(chunks):
        cut = slice(c * rows, (c + 1) * rows)
        swap(mine1, theirs1, s1, r1, c).wait_recv()
        summed = mine1[c].astype(jnp.float32) + theirs1[c].astype(jnp.float32)
        norm = layer_norm(states[cut, :].astype(jnp.float32) + summed, gain1[...])
        norm = norm.astype(jnp.bfloat16)
        normed[c] = norm
        v = dot(norm, up_w[...])
        hidden = (v * (1.0 + lax.erf(v * (0.5**0.5))) * 0.5).astype(jnp.bfloat16)
        mine2[c] = dot(hidden, down_w[...]).astype(mine2.dtype)
        swap(mine2, theirs2, s2, r2, c).start()
    for c in range(chunks):
        cut = slice(c * rows, (c + 1) * rows)
        swap(mine2, theirs2, s2, r2, c).wait_recv()
        summed = mine2[c].astype(jnp.float32) + theirs2[c].astype(jnp.float32)
        out[cut, :] = layer_norm(normed[c].astype(jnp.float32) + summed, gain2[...]).astype(
            jnp.bfloat16
        )
    for c in range(chunks):
        swap(mine1, theirs1, s1, r1, c).wait_send()
        swap(mine2, theirs2, s2, r2, c).wait_send()


def vmem_specs(count):
    return [pl.BlockSpec(memory_space=pltpu.VMEM)] * count


def shards(
    states,
    qkv_weight,
    out_weight,
    up_weight,
    down_weight,
    attn_gain,
    mlp_gain,
    global_ids,
    random_owner,
    random_local,
):
    tokens, width = states.shape
    heads = qkv_weight.shape[2] // HD
    pairs = heads // 2
    blocks = tokens // BS
    g_count = global_ids.shape[0]
    n = lax.axis_size("seq")

    owner = random_owner.reshape(-1)
    items = owner.shape[0]
    cap = max(2, items // n + 1)
    head_list = jnp.broadcast_to(
        jnp.arange(heads, dtype=jnp.int32)[None, :, None], (blocks, heads, R)
    ).reshape(-1)
    code = random_local.reshape(-1) * heads + head_list
    earlier = jnp.arange(items)[:, None] > jnp.arange(items)[None, :]
    rank = jnp.sum(((owner[:, None] == owner[None, :]) & earlier).astype(jnp.int32), axis=1)
    slot = owner * cap + rank
    place = owner * LANES + rank
    wanted = jnp.sum(
        jnp.where(
            place[None, None, :]
            == (jnp.arange(n)[:, None] * LANES + jnp.arange(LANES)[None, :])[:, :, None],
            code[None, None, :],
            0,
        ),
        axis=2,
    ).reshape(n, 1, LANES)

    units = g_count * (width // LANES) * (BS // 16)
    per = max(1, units // n)
    part_rows = heads * g_count * BS
    rows_per = -(-part_rows // n // 8) * 8
    bf, f32 = jnp.bfloat16, jnp.float32
    own = blocks * heads
    dma = pltpu.SemaphoreType.DMA
    att = pl.pallas_call(
        functools.partial(attend_kernel, n, cap, heads, blocks, g_count),
        out_shape=jax.ShapeDtypeStruct((pairs, tokens, LANES), bf),
        in_specs=vmem_specs(3) + [pl.BlockSpec(memory_space=pltpu.SMEM)] * 2,
        out_specs=pl.BlockSpec(memory_space=pltpu.VMEM),
        scratch_shapes=[
            pltpu.VMEM((n, 1, LANES), jnp.int32),
            pltpu.SMEM((n, 1, LANES), jnp.int32),
            pltpu.VMEM((units, 16, LANES), bf),
            pltpu.VMEM((n, per, 16, LANES), bf),
            pltpu.VMEM((per, 16, LANES), bf),
            pltpu.VMEM((units, 16, LANES), bf),
            pltpu.VMEM((g_count * BS, width), bf),
            pltpu.VMEM((own, BS, LANES), bf),
            pltpu.VMEM((own, BS, LANES), bf),
            pltpu.VMEM((n * cap, BS, LANES), bf),
            pltpu.VMEM((n * cap, BS, LANES), bf),
            pltpu.VMEM((heads, BS, LANES), bf),
            pltpu.VMEM((heads, BS, LANES), bf),
            pltpu.VMEM((own + 2 * heads, BS, LANES), bf),
            pltpu.VMEM((heads, g_count * BS, LANES), bf),
            pltpu.VMEM((heads, g_count * BS, LANES), bf),
            pltpu.VMEM((part_rows, LANES), f32),
            pltpu.VMEM((n, rows_per, LANES), f32),
            pltpu.VMEM((rows_per, LANES), f32),
            pltpu.VMEM((part_rows, LANES), f32),
        ]
        + [dma((n,))] * 8
        + [dma((2,))] * 2
        + [dma((n,))] * 4
        + [dma(())],
        compiler_params=pltpu.CompilerParams(
            collective_id=0, has_side_effects=True, vmem_limit_bytes=32 * 1024 * 1024
        ),
    )(states, qkv_weight, wanted, slot, global_ids)

    chunks = 4
    rows = tokens // chunks
    link = jnp.bfloat16
    return pl.pallas_call(
        functools.partial(tail_kernel, chunks),
        out_shape=jax.ShapeDtypeStruct((tokens, width), bf),
        in_specs=vmem_specs(7),
        out_specs=pl.BlockSpec(memory_space=pltpu.VMEM),
        scratch_shapes=[pltpu.VMEM((chunks, rows, width), link)] * 4
        + [dma((chunks,))] * 4
        + [pltpu.VMEM((chunks, rows, width), bf)],
        compiler_params=pltpu.CompilerParams(
            collective_id=1, has_side_effects=True, vmem_limit_bytes=32 * 1024 * 1024
        ),
    )(
        att,
        states,
        out_weight,
        up_weight,
        down_weight,
        attn_gain.reshape(1, width),
        mlp_gain.reshape(1, width),
    )


def solution(mesh):
    in_specs = (
        P("seq", None),
        P(None, None, "mp"),
        P("mp", None),
        P(None, "mp"),
        P("mp", None),
        P(),
        P(),
        P(),
        P("mp", "seq", None, None),
        P("mp", "seq", None, None),
    )
    out_specs = P("seq", None)
    return jax.shard_map(shards, mesh=mesh, in_specs=in_specs, out_specs=out_specs, check_vma=False)
```

```python
import functools

import jax
import jax.numpy as jnp
from jax import lax
from jax.experimental import pallas as pl
from jax.experimental.pallas import tpu as pltpu
from jax.sharding import PartitionSpec as P

HD = 64
BS = 64
R = 3
LANES = 128
MESH = pl.DeviceIdType.MESH

EPSILON = 1e-05
NEGATIVE = -1e30


def layer_norm(inputs, scales):
    center = jnp.mean(inputs, axis=-1, keepdims=True)
    shifted = inputs - center
    spread = jnp.mean(shifted * shifted, axis=-1, keepdims=True)
    return shifted * lax.rsqrt(spread + EPSILON) * scales


def dot_t(a, b):
    return lax.dot_general(a, b, (((1,), (1,)), ((), ())), preferred_element_type=jnp.float32)


def dot(a, b):
    return jnp.dot(a, b, preferred_element_type=jnp.float32)


def swap_halves(x):
    return pltpu.roll(x, HD, 1)


def attend_kernel(
    n,
    cap,
    heads,
    blocks,
    g_count,
    states_hbm,
    weight_hbm,
    wanted,
    slot,
    gids,
    att,
    states,
    weight,
    tab,
    tab_s,
    cand,
    cand_in,
    pick,
    gath,
    gstates,
    kvb,
    qpad,
    stage,
    rr,
    halo_l,
    halo_r,
    win,
    gq,
    gkv,
    part,
    part_in,
    gmine,
    gout,
    s_tab,
    r_tab,
    s_cand,
    r_cand,
    s_gath,
    r_gath,
    s_rand,
    r_rand,
    s_halo,
    r_halo,
    s_part,
    r_part,
    s_gout,
    r_gout,
    s_mp,
    r_mp,
    l_sem,
    w_sem,
):
    me = lax.axis_index("seq")
    mine = lax.axis_index("mp")
    pairs = heads // 2
    width = states.shape[1]
    cols = width // LANES
    quarters = BS // 16
    half = gath.shape[0]
    gper = gath.shape[1] // (cols * quarters)
    units = gper * cols * quarters
    per = cand_in.shape[1]
    cand_parts = units // per
    rows_per = part_in.shape[2]
    part_parts = part.shape[0]
    left = lax.rem(me + n - 1, n)
    right = lax.rem(me + 1, n)

    def peer(k):
        return lax.rem(me + k, n)

    def each_peer(body):
        def step(k, carry):
            body(peer(k))
            return carry

        lax.fori_loop(1, n, step, 0)

    def guarded(limit, who, body):
        if limit < n:
            pl.when(who < limit)(body)
        else:
            body()

    def remote(src, dst, ssem, rsem, d):
        return pltpu.make_async_remote_copy(
            src_ref=src,
            dst_ref=dst,
            send_sem=ssem,
            recv_sem=rsem,
            device_id={"seq": d},
            device_id_type=MESH,
        )

    def tab_copy(d, owner):
        return remote(wanted.at[d], tab.at[owner], s_tab.at[d], r_tab.at[owner], d)

    def cand_copy(d, owner, at):
        return remote(
            cand.at[pl.ds(at * per, per)], cand_in.at[owner], s_cand.at[d], r_cand.at[owner], d
        )

    def gath_copy(d, owner):
        return remote(
            pick, gath.at[mine, pl.ds(owner * per, per)], s_gath.at[d], r_gath.at[owner], d
        )

    def rand_copy(d, owner):
        return remote(
            stage.at[pl.ds(d * cap, cap)],
            rr.at[pl.ds(owner * cap, cap)],
            s_rand.at[d],
            r_rand.at[owner],
            d,
        )

    def part_copy(d, owner, at):
        return remote(part.at[at], part_in.at[owner], s_part.at[d], r_part.at[owner], d)

    def gout_copy(d, owner):
        return remote(gmine, gout.at[owner], s_gout.at[d], r_gout.at[owner], d)

    def mp_copy(k, owner):
        other = lax.rem(mine + k, half)
        return pltpu.make_async_remote_copy(
            src_ref=gath.at[mine],
            dst_ref=gath.at[owner],
            send_sem=s_mp.at[k],
            recv_sem=r_mp.at[owner],
            device_id={"mp": other},
            device_id_type=MESH,
        )

    to_right = remote(
        kvb.at[pl.ds((blocks - 1) * heads, heads)], halo_l, s_halo.at[0], r_halo.at[0], right
    )
    to_left = remote(kvb.at[pl.ds(0, heads)], halo_r, s_halo.at[1], r_halo.at[1], left)

    loads = [pltpu.make_async_copy(states_hbm, states, w_sem.at[3])] + [
        pltpu.make_async_copy(weight_hbm.at[i], weight.at[i], w_sem.at[i]) for i in (1, 2, 0)
    ]
    for load in loads:
        load.start()

    barrier = pltpu.get_barrier_semaphore()
    each_peer(
        lambda d: pl.semaphore_signal(barrier, inc=1, device_id={"seq": d}, device_id_type=MESH)
    )
    for k in range(1, half):
        pl.semaphore_signal(
            barrier, inc=1, device_id={"mp": lax.rem(mine + k, half)}, device_id_type=MESH
        )

    loads[0].wait()
    for i in range(gper):
        local = lax.rem(gids[mine * gper + i], blocks)
        for j in range(cols):
            cut = slice(j * LANES, (j + 1) * LANES)
            piece = states[0:BS, cut]
            for b in range(1, blocks):
                piece = jnp.where(local == b, states[b * BS : (b + 1) * BS, cut], piece)
            for q in range(quarters):
                cand[(i * cols + j) * quarters + q] = piece[q * 16 : (q + 1) * 16]
    tab[me] = wanted[me]

    def own_cand():
        cand_in[me] = cand[pl.ds(me * per, per)]

    guarded(cand_parts, me, own_cand)
    loads[1].wait()
    loads[2].wait()

    lane = lax.broadcasted_iota(jnp.int32, (BS, LANES), 1)
    low = lane < HD
    x = states[...]
    for j in range(pairs):
        cut = slice(j * LANES, (j + 1) * LANES)
        k = dot(x, weight[1, :, cut])
        v = dot(x, weight[2, :, cut])
        for b in range(blocks):
            kb, vb = k[b * BS : (b + 1) * BS], v[b * BS : (b + 1) * BS]
            kvb[b * heads + 2 * j] = jnp.where(low, kb, swap_halves(vb)).astype(jnp.bfloat16)
            kvb[b * heads + 2 * j + 1] = jnp.where(low, swap_halves(kb), vb).astype(jnp.bfloat16)

    pl.semaphore_wait(barrier, n - 1 + half - 1)
    each_peer(lambda d: tab_copy(d, me).start())
    each_peer(lambda d: guarded(cand_parts, d, lambda: cand_copy(d, me, d).start()))
    to_right.start()
    to_left.start()

    loads[3].wait()
    scaling = HD ** (-0.5)
    for j in range(pairs):
        cut = slice(j * LANES, (j + 1) * LANES)
        q = dot(x, weight[0, :, cut]).astype(jnp.bfloat16).astype(jnp.float32) * scaling
        for b in range(blocks):
            qb = q[b * BS : (b + 1) * BS]
            qpad[b * heads + 2 * j] = jnp.where(low, qb, 0.0).astype(jnp.bfloat16)
            qpad[b * heads + 2 * j + 1] = jnp.where(low, swap_halves(qb), 0.0).astype(jnp.bfloat16)

    each_peer(lambda d: tab_copy(d, d).wait_recv())
    table = pltpu.make_async_copy(tab, tab_s, l_sem)
    table.start()
    table.wait()

    def serve(d):
        for c in range(cap):
            stage[d * cap + c] = kvb[tab_s[d, 0, c]]
        rand_copy(d, me).start()

    def serve_some(start, stop):
        def step(k, carry):
            serve(peer(k))
            return carry

        lax.fori_loop(start, stop, step, 0)

    batch = 1 + n // 3
    serve_some(1, batch)
    for c in range(cap):
        rr[me * cap + c] = kvb[tab_s[me, 0, c]]

    def relay():
        each_peer(lambda d: cand_copy(d, d, me).wait_recv())
        for u in range(per):
            g = (me * per + u) // (cols * quarters)
            wanted_id = gids[mine * gper + g]

            def choose(d, so_far):
                here = (wanted_id >= d * blocks) & (wanted_id < (d + 1) * blocks)
                return jnp.where(here, cand_in[d, u], so_far)

            pick[u] = lax.fori_loop(1, n, choose, cand_in[0, u])
        gath[mine, pl.ds(me * per, per)] = pick[...]
        each_peer(lambda d: gath_copy(d, me).start())

    guarded(cand_parts, me, relay)

    each_peer(lambda d: guarded(cand_parts, d, lambda: gath_copy(d, d).wait_recv()))
    for k in range(1, half):
        mp_copy(k, mine).start()
    for k in range(1, half):
        mp_copy(k, lax.rem(mine + k, half)).wait_recv()
    for g in range(g_count):
        for j in range(cols):
            for q in range(quarters):
                gstates[g * BS + q * 16 : g * BS + (q + 1) * 16, j * LANES : (j + 1) * LANES] = (
                    gath[g // gper, ((g % gper) * cols + j) * quarters + q]
                )
    gx = gstates[...]
    rows = g_count * BS
    glane = lax.broadcasted_iota(jnp.int32, (rows, LANES), 1)
    glow = glane < HD
    for j in range(pairs):
        cut = slice(j * LANES, (j + 1) * LANES)
        q = dot(gx, weight[0, :, cut]).astype(jnp.bfloat16).astype(jnp.float32) * scaling
        k = dot(gx, weight[1, :, cut])
        v = dot(gx, weight[2, :, cut])
        gq[2 * j] = jnp.where(glow, q, 0.0).astype(jnp.bfloat16)
        gq[2 * j + 1] = jnp.where(glow, swap_halves(q), 0.0).astype(jnp.bfloat16)
        gkv[2 * j] = jnp.where(glow, k, swap_halves(v)).astype(jnp.bfloat16)
        gkv[2 * j + 1] = jnp.where(glow, swap_halves(k), v).astype(jnp.bfloat16)

    for h in range(heads):
        keys = jnp.concatenate([kvb[b * heads + h] for b in range(blocks)], axis=0)
        s = dot_t(gq[h], keys)
        high = jnp.max(s, axis=-1, keepdims=True)
        e = jnp.exp(s - high)
        total = jnp.sum(e, axis=-1, keepdims=True)
        e_high = e.astype(jnp.bfloat16)
        e_low = (e - e_high.astype(jnp.float32)).astype(jnp.bfloat16)
        acc = (dot(e_high, keys) + dot(e_low, keys)) * (1.0 / total)
        level = high + jnp.log(total)
        first = level.astype(jnp.bfloat16).astype(jnp.float32)
        second = (level - first).astype(jnp.bfloat16).astype(jnp.float32)
        third = level - first - second
        packed = jnp.where(
            glane < 16,
            first,
            jnp.where(glane < 32, second, jnp.where(glow, third, acc)),
        ).astype(jnp.bfloat16)
        cuts = rows // rows_per
        for c in range(cuts):
            part[(h // 2) * cuts + c, h % 2] = packed[c * rows_per : (c + 1) * rows_per]
    each_peer(lambda d: guarded(part_parts, d, lambda: part_copy(d, me, d).start()))
    serve_some(batch, n)

    to_right.wait_recv()
    to_left.wait_recv()
    win[0:heads] = halo_l[...]
    win[heads : heads + blocks * heads] = kvb[...]
    win[heads + blocks * heads :] = halo_r[...]

    def combine():
        part_in[me] = part[me]
        each_peer(lambda d: part_copy(d, d, me).wait_recv())
        outs = []
        for parity in range(2):

            def level(d):
                piece = part_in[d, parity].astype(jnp.float32)
                return piece, piece[:, 0:1] + piece[:, 16:17] + piece[:, 32:33]

            def top(d, best):
                return jnp.maximum(best, level(d)[1])

            best = lax.fori_loop(1, n, top, level(0)[1])

            def add(d, so_far):
                piece, high = level(d)
                factor = jnp.exp(high - best)
                return so_far[0] + piece * factor, so_far[1] + factor

            zero = (jnp.zeros((rows_per, LANES), jnp.float32), jnp.zeros((rows_per, 1), jnp.float32))
            summed, total = lax.fori_loop(0, n, add, zero)
            outs.append(summed / total)
        plow = lax.broadcasted_iota(jnp.int32, (rows_per, LANES), 1) < HD
        done = jnp.where(plow, swap_halves(outs[0]), outs[1]).astype(jnp.bfloat16)
        gmine[...] = done
        gout[me] = done
        each_peer(lambda d: gout_copy(d, me).start())

    guarded(part_parts, me, combine)

    each_peer(lambda d: rand_copy(d, d).wait_recv())

    slots = 3 + R + g_count
    slot_lane = lax.broadcasted_iota(jnp.int32, (BS, slots * BS), 1)

    def block_step(b, carry):
        first = me * blocks + b
        start = jnp.where(first == 0, BS, 0)
        stop = jnp.where(first == n * blocks - 1, 2 * BS, 3 * BS)
        outside = (slot_lane < start) | ((slot_lane >= stop) & (slot_lane < 3 * BS))
        for j in range(pairs):
            halves = []
            for h in (2 * j, 2 * j + 1):
                at = b * heads + h
                keys = jnp.concatenate(
                    [win[at + t * heads] for t in range(3)]
                    + [rr[slot[at * R + r]] for r in range(R)]
                    + [gkv[h]],
                    axis=0,
                )
                s = jnp.where(outside, NEGATIVE, dot_t(qpad[at], keys))
                e = jnp.exp(s - jnp.max(s, axis=-1, keepdims=True))
                w = (e * (1.0 / jnp.sum(e, axis=-1, keepdims=True))).astype(jnp.bfloat16)
                halves.append(dot(w, keys))
            att[j, pl.ds(pl.multiple_of(b * BS, BS), BS), :] = jnp.where(
                low, swap_halves(halves[0]), halves[1]
            ).astype(jnp.bfloat16)
        return carry

    lax.fori_loop(0, blocks, block_step, 0)

    each_peer(lambda d: guarded(part_parts, d, lambda: gout_copy(d, d).wait_recv()))
    for j in range(pairs):
        for g in range(g_count):
            cuts = BS // rows_per
            at = (j * g_count + g) * cuts
            row = jnp.concatenate([gout[at + c] for c in range(cuts)], axis=0).astype(jnp.float32)
            for b in range(blocks):
                here = gids[g] == me * blocks + b
                old = att[j, b * BS : (b + 1) * BS, :].astype(jnp.float32)
                att[j, b * BS : (b + 1) * BS, :] = jnp.where(here, row, old).astype(jnp.bfloat16)

    def drain(d):
        tab_copy(d, me).wait_send()
        guarded(cand_parts, d, lambda: cand_copy(d, me, d).wait_send())
        guarded(cand_parts, me, lambda: gath_copy(d, me).wait_send())
        rand_copy(d, me).wait_send()
        guarded(part_parts, d, lambda: part_copy(d, me, d).wait_send())
        guarded(part_parts, me, lambda: gout_copy(d, me).wait_send())

    each_peer(drain)
    for k in range(1, half):
        mp_copy(k, mine).wait_send()
    to_right.wait_send()
    to_left.wait_send()


def tail_kernel(
    chunks,
    att,
    states,
    out_w,
    up_w,
    down_w,
    gain1,
    gain2,
    out,
    mine1,
    theirs1,
    mine2,
    theirs2,
    s1,
    r1,
    s2,
    r2,
    normed,
):
    other = 1 - lax.axis_index("mp")
    barrier = pltpu.get_barrier_semaphore()
    pl.semaphore_signal(barrier, inc=1, device_id={"mp": other}, device_id_type=MESH)
    pl.semaphore_wait(barrier, 1)
    rows = states.shape[0] // chunks

    def swap(mine, theirs, ssem, rsem, c):
        return pltpu.make_async_remote_copy(
            src_ref=mine.at[c],
            dst_ref=theirs.at[c],
            send_sem=ssem.at[c],
            recv_sem=rsem.at[c],
            device_id={"mp": other},
            device_id_type=MESH,
        )

    for c in range(chunks):
        cut = slice(c * rows, (c + 1) * rows)
        acc = dot(att[0, cut, :], out_w[0:LANES, :])
        for j in range(1, att.shape[0]):
            acc = acc + dot(att[j, cut, :], out_w[j * LANES : (j + 1) * LANES, :])
        mine1[c] = acc.astype(mine1.dtype)
        swap(mine1, theirs1, s1, r1, c).start()
    for c in range(chunks):
        cut = slice(c * rows, (c + 1) * rows)
        swap(mine1, theirs1, s1, r1, c).wait_recv()
        summed = mine1[c].astype(jnp.float32) + theirs1[c].astype(jnp.float32)
        norm = layer_norm(states[cut, :].astype(jnp.float32) + summed, gain1[...])
        norm = norm.astype(jnp.bfloat16)
        normed[c] = norm
        v = dot(norm, up_w[...])
        hidden = (v * (1.0 + lax.erf(v * (0.5**0.5))) * 0.5).astype(jnp.bfloat16)
        mine2[c] = dot(hidden, down_w[...]).astype(mine2.dtype)
        swap(mine2, theirs2, s2, r2, c).start()
    for c in range(chunks):
        cut = slice(c * rows, (c + 1) * rows)
        swap(mine2, theirs2, s2, r2, c).wait_recv()
        summed = mine2[c].astype(jnp.float32) + theirs2[c].astype(jnp.float32)
        out[cut, :] = layer_norm(normed[c].astype(jnp.float32) + summed, gain2[...]).astype(
            jnp.bfloat16
        )
    for c in range(chunks):
        swap(mine1, theirs1, s1, r1, c).wait_send()
        swap(mine2, theirs2, s2, r2, c).wait_send()


def vmem_specs(count):
    return [pl.BlockSpec(memory_space=pltpu.VMEM)] * count


def shards(
    states,
    qkv_weight,
    out_weight,
    up_weight,
    down_weight,
    attn_gain,
    mlp_gain,
    global_ids,
    random_owner,
    random_local,
):
    tokens, width = states.shape
    heads = qkv_weight.shape[2] // HD
    pairs = heads // 2
    blocks = tokens // BS
    g_count = global_ids.shape[0]
    n = lax.axis_size("seq")

    owner = random_owner.reshape(-1)
    items = owner.shape[0]
    cap = max(2, items // n + 1)
    head_list = jnp.broadcast_to(
        jnp.arange(heads, dtype=jnp.int32)[None, :, None], (blocks, heads, R)
    ).reshape(-1)
    code = random_local.reshape(-1) * heads + head_list
    earlier = jnp.arange(items)[:, None] > jnp.arange(items)[None, :]
    rank = jnp.sum(((owner[:, None] == owner[None, :]) & earlier).astype(jnp.int32), axis=1)
    slot = owner * cap + rank
    place = owner * LANES + rank
    wanted = jnp.sum(
        jnp.where(
            place[None, None, :]
            == (jnp.arange(n)[:, None] * LANES + jnp.arange(LANES)[None, :])[:, :, None],
            code[None, None, :],
            0,
        ),
        axis=2,
    ).reshape(n, 1, LANES)

    half = lax.axis_size("mp")
    units = (g_count // half) * (width // LANES) * (BS // 16)
    per = -(-units // n)
    part_rows = pairs * g_count * BS
    rows_per = -(-part_rows // n // 16) * 16
    parts = part_rows // rows_per
    bf = jnp.bfloat16
    own = blocks * heads
    dma = pltpu.SemaphoreType.DMA
    att = pl.pallas_call(
        functools.partial(attend_kernel, n, cap, heads, blocks, g_count),
        out_shape=jax.ShapeDtypeStruct((pairs, tokens, LANES), bf),
        in_specs=[pl.BlockSpec(memory_space=pltpu.HBM)] * 2
        + vmem_specs(1)
        + [pl.BlockSpec(memory_space=pltpu.SMEM)] * 2,
        out_specs=pl.BlockSpec(memory_space=pltpu.VMEM),
        scratch_shapes=[
            pltpu.VMEM((tokens, width), bf),
            pltpu.VMEM(qkv_weight.shape, bf),
            pltpu.VMEM((n, 1, LANES), jnp.int32),
            pltpu.SMEM((n, 1, LANES), jnp.int32),
            pltpu.VMEM((units, 16, LANES), bf),
            pltpu.VMEM((n, per, 16, LANES), bf),
            pltpu.VMEM((per, 16, LANES), bf),
            pltpu.VMEM((half, units, 16, LANES), bf),
            pltpu.VMEM((g_count * BS, width), bf),
            pltpu.VMEM((own, BS, LANES), bf),
            pltpu.VMEM((own, BS, LANES), bf),
            pltpu.VMEM((n * cap, BS, LANES), bf),
            pltpu.VMEM((n * cap, BS, LANES), bf),
            pltpu.VMEM((heads, BS, LANES), bf),
            pltpu.VMEM((heads, BS, LANES), bf),
            pltpu.VMEM((own + 2 * heads, BS, LANES), bf),
            pltpu.VMEM((heads, g_count * BS, LANES), bf),
            pltpu.VMEM((heads, g_count * BS, LANES), bf),
            pltpu.VMEM((parts, 2, rows_per, LANES), bf),
            pltpu.VMEM((n, 2, rows_per, LANES), bf),
            pltpu.VMEM((rows_per, LANES), bf),
            pltpu.VMEM((parts, rows_per, LANES), bf),
        ]
        + [dma((n,))] * 8
        + [dma((2,))] * 2
        + [dma((n,))] * 4
        + [dma((half,))] * 2
        + [dma(()), dma((4,))],
        cost_estimate=pl.CostEstimate(
            flops=30_000_000_000, bytes_accessed=20_000_000, transcendentals=0
        ),
        compiler_params=pltpu.CompilerParams(
            collective_id=0, has_side_effects=True, vmem_limit_bytes=32 * 1024 * 1024
        ),
    )(
        pltpu.with_memory_space_constraint(states, pltpu.HBM),
        pltpu.with_memory_space_constraint(qkv_weight, pltpu.HBM),
        wanted,
        slot,
        global_ids,
    )

    chunks = 4
    rows = tokens // chunks
    link = jnp.bfloat16
    return pl.pallas_call(
        functools.partial(tail_kernel, chunks),
        out_shape=jax.ShapeDtypeStruct((tokens, width), bf),
        in_specs=vmem_specs(7),
        out_specs=pl.BlockSpec(memory_space=pltpu.VMEM),
        scratch_shapes=[pltpu.VMEM((chunks, rows, width), link)] * 4
        + [dma((chunks,))] * 4
        + [pltpu.VMEM((chunks, rows, width), bf)],
        compiler_params=pltpu.CompilerParams(
            collective_id=1, has_side_effects=True, vmem_limit_bytes=32 * 1024 * 1024
        ),
    )(
        att,
        states,
        out_weight,
        up_weight,
        down_weight,
        attn_gain.reshape(1, width),
        mlp_gain.reshape(1, width),
    )


def solution(mesh):
    in_specs = (
        P("seq", None),
        P(None, None, "mp"),
        P("mp", None),
        P(None, "mp"),
        P("mp", None),
        P(),
        P(),
        P(),
        P("mp", "seq", None, None),
        P("mp", "seq", None, None),
    )
    out_specs = P("seq", None)
    return jax.shard_map(shards, mesh=mesh, in_specs=in_specs, out_specs=out_specs, check_vma=False)
```

```python
import functools

import jax
import jax.numpy as jnp
from jax import lax
from jax.experimental import pallas as pl
from jax.experimental.pallas import tpu as pltpu
from jax.sharding import PartitionSpec as P

HD = 64
BS = 64
R = 3
LANES = 128
MESH = pl.DeviceIdType.MESH

EPSILON = 1e-05
NEGATIVE = -1e30


def layer_norm(inputs, scales):
    center = jnp.mean(inputs, axis=-1, keepdims=True)
    shifted = inputs - center
    spread = jnp.mean(shifted * shifted, axis=-1, keepdims=True)
    return shifted * lax.rsqrt(spread + EPSILON) * scales


def dot_t(a, b):
    return lax.dot_general(a, b, (((1,), (1,)), ((), ())), preferred_element_type=jnp.float32)


def dot(a, b):
    return jnp.dot(a, b, preferred_element_type=jnp.float32)


def swap_halves(x):
    return pltpu.roll(x, HD, 1)


def attend_kernel(
    n,
    cap,
    heads,
    blocks,
    g_count,
    states_hbm,
    weight_hbm,
    wanted,
    slot,
    gids,
    att,
    states,
    weight,
    tab,
    tab_s,
    cand,
    cand_in,
    pick,
    gath,
    gstates,
    kvb,
    qpad,
    stage,
    rr,
    halo_l,
    halo_r,
    win,
    gq,
    gkv,
    part,
    part_in,
    gmine,
    gout,
    scores,
    s_tab,
    r_tab,
    s_cand,
    r_cand,
    s_gath,
    r_gath,
    s_rand,
    r_rand,
    s_halo,
    r_halo,
    s_part,
    r_part,
    s_gout,
    r_gout,
    s_mp,
    r_mp,
    l_sem,
    w_sem,
):
    me = lax.axis_index("seq")
    mine = lax.axis_index("mp")
    pairs = heads // 2
    width = states.shape[1]
    cols = width // LANES
    quarters = BS // 16
    half = gath.shape[0]
    gper = gath.shape[1] // (cols * quarters)
    units = gper * cols * quarters
    per = cand_in.shape[1]
    cand_parts = units // per
    rows_per = part_in.shape[2]
    part_parts = part.shape[0]
    left = lax.rem(me + n - 1, n)
    right = lax.rem(me + 1, n)

    def peer(k):
        return lax.rem(me + k, n)

    def each_peer(body):
        def step(k, carry):
            body(peer(k))
            return carry

        lax.fori_loop(1, n, step, 0)

    def guarded(limit, who, body):
        if limit < n:
            pl.when(who < limit)(body)
        else:
            body()

    def remote(src, dst, ssem, rsem, d):
        return pltpu.make_async_remote_copy(
            src_ref=src,
            dst_ref=dst,
            send_sem=ssem,
            recv_sem=rsem,
            device_id={"seq": d},
            device_id_type=MESH,
        )

    def tab_copy(d, owner):
        return remote(wanted.at[d], tab.at[owner], s_tab.at[d], r_tab.at[owner], d)

    def cand_copy(d, owner, at):
        return remote(
            cand.at[pl.ds(at * per, per)], cand_in.at[owner], s_cand.at[d], r_cand.at[owner], d
        )

    def gath_copy(d, owner):
        return remote(
            pick, gath.at[mine, pl.ds(owner * per, per)], s_gath.at[d], r_gath.at[owner], d
        )

    def rand_copy(d, owner):
        return remote(
            stage.at[pl.ds(d * cap, cap)],
            rr.at[pl.ds(owner * cap, cap)],
            s_rand.at[d],
            r_rand.at[owner],
            d,
        )

    def part_copy(d, owner, at):
        return remote(part.at[at], part_in.at[owner], s_part.at[d], r_part.at[owner], d)

    def gout_copy(d, owner):
        return remote(gmine, gout.at[owner], s_gout.at[d], r_gout.at[owner], d)

    def mp_copy(k, owner):
        other = lax.rem(mine + k, half)
        return pltpu.make_async_remote_copy(
            src_ref=gath.at[mine],
            dst_ref=gath.at[owner],
            send_sem=s_mp.at[k],
            recv_sem=r_mp.at[owner],
            device_id={"mp": other},
            device_id_type=MESH,
        )

    to_right = remote(
        kvb.at[pl.ds((blocks - 1) * heads, heads)], halo_l, s_halo.at[0], r_halo.at[0], right
    )
    to_left = remote(kvb.at[pl.ds(0, heads)], halo_r, s_halo.at[1], r_halo.at[1], left)

    loads = [pltpu.make_async_copy(states_hbm, states, w_sem.at[3])] + [
        pltpu.make_async_copy(weight_hbm.at[i], weight.at[i], w_sem.at[i]) for i in (1, 2, 0)
    ]
    for load in loads:
        load.start()

    barrier = pltpu.get_barrier_semaphore()
    each_peer(
        lambda d: pl.semaphore_signal(barrier, inc=1, device_id={"seq": d}, device_id_type=MESH)
    )
    for k in range(1, half):
        pl.semaphore_signal(
            barrier, inc=1, device_id={"mp": lax.rem(mine + k, half)}, device_id_type=MESH
        )

    loads[0].wait()
    for i in range(gper):
        local = lax.rem(gids[mine * gper + i], blocks)
        for j in range(cols):
            cut = slice(j * LANES, (j + 1) * LANES)
            piece = states[0:BS, cut]
            for b in range(1, blocks):
                piece = jnp.where(local == b, states[b * BS : (b + 1) * BS, cut], piece)
            for q in range(quarters):
                cand[(i * cols + j) * quarters + q] = piece[q * 16 : (q + 1) * 16]
    tab[me] = wanted[me]

    def own_cand():
        cand_in[me] = cand[pl.ds(me * per, per)]

    guarded(cand_parts, me, own_cand)
    loads[1].wait()
    loads[2].wait()

    lane = lax.broadcasted_iota(jnp.int32, (BS, LANES), 1)
    low = lane < HD
    x = states[...]
    for j in range(pairs):
        cut = slice(j * LANES, (j + 1) * LANES)
        k = dot(x, weight[1, :, cut])
        v = dot(x, weight[2, :, cut])
        for b in range(blocks):
            kb, vb = k[b * BS : (b + 1) * BS], v[b * BS : (b + 1) * BS]
            kvb[b * heads + 2 * j] = jnp.where(low, kb, swap_halves(vb)).astype(jnp.bfloat16)
            kvb[b * heads + 2 * j + 1] = jnp.where(low, swap_halves(kb), vb).astype(jnp.bfloat16)

    pl.semaphore_wait(barrier, n - 1 + half - 1)
    each_peer(lambda d: tab_copy(d, me).start())
    each_peer(lambda d: guarded(cand_parts, d, lambda: cand_copy(d, me, d).start()))
    to_right.start()
    to_left.start()

    loads[3].wait()
    scaling = HD ** (-0.5)
    for j in range(pairs):
        cut = slice(j * LANES, (j + 1) * LANES)
        q = dot(x, weight[0, :, cut]).astype(jnp.bfloat16).astype(jnp.float32) * scaling
        for b in range(blocks):
            qb = q[b * BS : (b + 1) * BS]
            qpad[b * heads + 2 * j] = jnp.where(low, qb, 0.0).astype(jnp.bfloat16)
            qpad[b * heads + 2 * j + 1] = jnp.where(low, swap_halves(qb), 0.0).astype(jnp.bfloat16)

    def relay():
        each_peer(lambda d: cand_copy(d, d, me).wait_recv())
        for u in range(per):
            g = (me * per + u) // (cols * quarters)
            wanted_id = gids[mine * gper + g]

            def choose(d, so_far):
                here = (wanted_id >= d * blocks) & (wanted_id < (d + 1) * blocks)
                return jnp.where(here, cand_in[d, u], so_far)

            pick[u] = lax.fori_loop(1, n, choose, cand_in[0, u])
        gath[mine, pl.ds(me * per, per)] = pick[...]
        each_peer(lambda d: gath_copy(d, me).start())

    guarded(cand_parts, me, relay)

    each_peer(lambda d: tab_copy(d, d).wait_recv())
    table = pltpu.make_async_copy(tab, tab_s, l_sem)
    table.start()
    table.wait()

    def serve(d):
        for c in range(cap):
            stage[d * cap + c] = kvb[tab_s[d, 0, c]]
        rand_copy(d, me).start()

    def serve_some(start, stop):
        def step(k, carry):
            serve(peer(k))
            return carry

        lax.fori_loop(start, stop, step, 0)

    batch = n // 2
    serve_some(1, batch)
    for c in range(cap):
        rr[me * cap + c] = kvb[tab_s[me, 0, c]]

    each_peer(lambda d: guarded(cand_parts, d, lambda: gath_copy(d, d).wait_recv()))
    for k in range(1, half):
        mp_copy(k, mine).start()
    for k in range(1, half):
        mp_copy(k, lax.rem(mine + k, half)).wait_recv()
    for g in range(g_count):
        for j in range(cols):
            for q in range(quarters):
                gstates[g * BS + q * 16 : g * BS + (q + 1) * 16, j * LANES : (j + 1) * LANES] = (
                    gath[g // gper, ((g % gper) * cols + j) * quarters + q]
                )
    gx = gstates[...]
    rows = g_count * BS
    glane = lax.broadcasted_iota(jnp.int32, (rows, LANES), 1)
    glow = glane < HD
    for j in range(pairs):
        cut = slice(j * LANES, (j + 1) * LANES)
        q = dot(gx, weight[0, :, cut]).astype(jnp.bfloat16).astype(jnp.float32) * scaling
        k = dot(gx, weight[1, :, cut])
        v = dot(gx, weight[2, :, cut])
        gq[2 * j] = jnp.where(glow, q, 0.0).astype(jnp.bfloat16)
        gq[2 * j + 1] = jnp.where(glow, swap_halves(q), 0.0).astype(jnp.bfloat16)
        gkv[2 * j] = jnp.where(glow, k, swap_halves(v)).astype(jnp.bfloat16)
        gkv[2 * j + 1] = jnp.where(glow, swap_halves(k), v).astype(jnp.bfloat16)

    for h in range(heads):
        keys = jnp.concatenate([kvb[b * heads + h] for b in range(blocks)], axis=0)
        s = dot_t(gq[h], keys)
        high = jnp.max(s, axis=-1, keepdims=True)
        e = jnp.exp(s - high)
        total = jnp.sum(e, axis=-1, keepdims=True)
        e_high = e.astype(jnp.bfloat16)
        e_low = (e - e_high.astype(jnp.float32)).astype(jnp.bfloat16)
        acc = (dot(e_high, keys) + dot(e_low, keys)) * (1.0 / total)
        level = high + jnp.log(total)
        first = level.astype(jnp.bfloat16).astype(jnp.float32)
        second = (level - first).astype(jnp.bfloat16).astype(jnp.float32)
        third = level - first - second
        packed = jnp.where(
            glane < 16,
            first,
            jnp.where(glane < 32, second, jnp.where(glow, third, acc)),
        ).astype(jnp.bfloat16)
        cuts = rows // rows_per
        for c in range(cuts):
            part[(h // 2) * cuts + c, h % 2] = packed[c * rows_per : (c + 1) * rows_per]
    each_peer(lambda d: guarded(part_parts, d, lambda: part_copy(d, me, d).start()))
    serve_some(batch, n)

    to_right.wait_recv()
    to_left.wait_recv()
    win[0:heads] = halo_l[...]
    win[heads : heads + blocks * heads] = kvb[...]
    win[heads + blocks * heads :] = halo_r[...]

    near = 3 + g_count
    slot_lane = lax.broadcasted_iota(jnp.int32, (BS, near * BS), 1)

    def near_keys(at, h):
        return jnp.concatenate([win[at + t * heads] for t in range(3)] + [gkv[h]], axis=0)

    def near_step(b, carry):
        first = me * blocks + b
        start = jnp.where(first == 0, BS, 0)
        stop = jnp.where(first == n * blocks - 1, 2 * BS, 3 * BS)
        outside = (slot_lane < start) | ((slot_lane >= stop) & (slot_lane < 3 * BS))
        for h in range(heads):
            at = b * heads + h
            scores[at] = jnp.where(outside, NEGATIVE, dot_t(qpad[at], near_keys(at, h)))
        return carry

    lax.fori_loop(0, blocks, near_step, 0)

    def combine():
        part_in[me] = part[me]
        each_peer(lambda d: part_copy(d, d, me).wait_recv())
        outs = []
        for parity in range(2):

            def level(d):
                piece = part_in[d, parity].astype(jnp.float32)
                return piece, piece[:, 0:1] + piece[:, 16:17] + piece[:, 32:33]

            def top(d, best):
                return jnp.maximum(best, level(d)[1])

            best = lax.fori_loop(1, n, top, level(0)[1])

            def add(d, so_far):
                piece, high = level(d)
                factor = jnp.exp(high - best)
                return so_far[0] + piece * factor, so_far[1] + factor

            zero = (jnp.zeros((rows_per, LANES), jnp.float32), jnp.zeros((rows_per, 1), jnp.float32))
            summed, total = lax.fori_loop(0, n, add, zero)
            outs.append(summed / total)
        plow = lax.broadcasted_iota(jnp.int32, (rows_per, LANES), 1) < HD
        done = jnp.where(plow, swap_halves(outs[0]), outs[1]).astype(jnp.bfloat16)
        gmine[...] = done
        gout[me] = done
        each_peer(lambda d: gout_copy(d, me).start())

    guarded(part_parts, me, combine)

    each_peer(lambda d: rand_copy(d, d).wait_recv())

    def block_step(b, carry):
        for j in range(pairs):
            halves = []
            for h in (2 * j, 2 * j + 1):
                at = b * heads + h
                early_keys = near_keys(at, h)
                keys = jnp.concatenate([rr[slot[at * R + r]] for r in range(R)], axis=0)
                s = dot_t(qpad[at], keys)
                early_s = scores[at]
                high = jnp.maximum(
                    jnp.max(s, axis=-1, keepdims=True), jnp.max(early_s, axis=-1, keepdims=True)
                )
                e = jnp.exp(s - high)
                early_e = jnp.exp(early_s - high)
                total = jnp.sum(e, axis=-1, keepdims=True) + jnp.sum(
                    early_e, axis=-1, keepdims=True
                )
                share = 1.0 / total
                w = (e * share).astype(jnp.bfloat16)
                early_w = (early_e * share).astype(jnp.bfloat16)
                halves.append(dot(w, keys) + dot(early_w, early_keys))
            att[j, pl.ds(pl.multiple_of(b * BS, BS), BS), :] = jnp.where(
                low, swap_halves(halves[0]), halves[1]
            ).astype(jnp.bfloat16)
        return carry

    lax.fori_loop(0, blocks, block_step, 0)

    each_peer(lambda d: guarded(part_parts, d, lambda: gout_copy(d, d).wait_recv()))
    for j in range(pairs):
        for g in range(g_count):
            cuts = BS // rows_per
            at = (j * g_count + g) * cuts
            row = jnp.concatenate([gout[at + c] for c in range(cuts)], axis=0).astype(jnp.float32)
            for b in range(blocks):
                here = gids[g] == me * blocks + b
                old = att[j, b * BS : (b + 1) * BS, :].astype(jnp.float32)
                att[j, b * BS : (b + 1) * BS, :] = jnp.where(here, row, old).astype(jnp.bfloat16)

    def drain(d):
        tab_copy(d, me).wait_send()
        guarded(cand_parts, d, lambda: cand_copy(d, me, d).wait_send())
        guarded(cand_parts, me, lambda: gath_copy(d, me).wait_send())
        rand_copy(d, me).wait_send()
        guarded(part_parts, d, lambda: part_copy(d, me, d).wait_send())
        guarded(part_parts, me, lambda: gout_copy(d, me).wait_send())

    each_peer(drain)
    for k in range(1, half):
        mp_copy(k, mine).wait_send()
    to_right.wait_send()
    to_left.wait_send()


def tail_kernel(
    chunks,
    att,
    states,
    out_w,
    up_w,
    down_w,
    gain1,
    gain2,
    out,
    mine1,
    theirs1,
    mine2,
    theirs2,
    s1,
    r1,
    s2,
    r2,
    normed,
):
    other = 1 - lax.axis_index("mp")
    barrier = pltpu.get_barrier_semaphore()
    pl.semaphore_signal(barrier, inc=1, device_id={"mp": other}, device_id_type=MESH)
    pl.semaphore_wait(barrier, 1)
    rows = states.shape[0] // chunks

    def swap(mine, theirs, ssem, rsem, c):
        return pltpu.make_async_remote_copy(
            src_ref=mine.at[c],
            dst_ref=theirs.at[c],
            send_sem=ssem.at[c],
            recv_sem=rsem.at[c],
            device_id={"mp": other},
            device_id_type=MESH,
        )

    for c in range(chunks):
        cut = slice(c * rows, (c + 1) * rows)
        acc = dot(att[0, cut, :], out_w[0:LANES, :])
        for j in range(1, att.shape[0]):
            acc = acc + dot(att[j, cut, :], out_w[j * LANES : (j + 1) * LANES, :])
        mine1[c] = acc.astype(mine1.dtype)
        swap(mine1, theirs1, s1, r1, c).start()
    for c in range(chunks):
        cut = slice(c * rows, (c + 1) * rows)
        swap(mine1, theirs1, s1, r1, c).wait_recv()
        summed = mine1[c].astype(jnp.float32) + theirs1[c].astype(jnp.float32)
        norm = layer_norm(states[cut, :].astype(jnp.float32) + summed, gain1[...])
        norm = norm.astype(jnp.bfloat16)
        normed[c] = norm
        v = dot(norm, up_w[...])
        hidden = (v * (1.0 + lax.erf(v * (0.5**0.5))) * 0.5).astype(jnp.bfloat16)
        mine2[c] = dot(hidden, down_w[...]).astype(mine2.dtype)
        swap(mine2, theirs2, s2, r2, c).start()
    for c in range(chunks):
        cut = slice(c * rows, (c + 1) * rows)
        swap(mine2, theirs2, s2, r2, c).wait_recv()
        summed = mine2[c].astype(jnp.float32) + theirs2[c].astype(jnp.float32)
        out[cut, :] = layer_norm(normed[c].astype(jnp.float32) + summed, gain2[...]).astype(
            jnp.bfloat16
        )
    for c in range(chunks):
        swap(mine1, theirs1, s1, r1, c).wait_send()
        swap(mine2, theirs2, s2, r2, c).wait_send()


def vmem_specs(count):
    return [pl.BlockSpec(memory_space=pltpu.VMEM)] * count


def shards(
    states,
    qkv_weight,
    out_weight,
    up_weight,
    down_weight,
    attn_gain,
    mlp_gain,
    global_ids,
    random_owner,
    random_local,
):
    tokens, width = states.shape
    heads = qkv_weight.shape[2] // HD
    pairs = heads // 2
    blocks = tokens // BS
    g_count = global_ids.shape[0]
    n = lax.axis_size("seq")

    owner = random_owner.reshape(-1)
    items = owner.shape[0]
    cap = max(2, items // n + 1)
    head_list = jnp.broadcast_to(
        jnp.arange(heads, dtype=jnp.int32)[None, :, None], (blocks, heads, R)
    ).reshape(-1)
    code = random_local.reshape(-1) * heads + head_list
    earlier = jnp.arange(items)[:, None] > jnp.arange(items)[None, :]
    rank = jnp.sum(((owner[:, None] == owner[None, :]) & earlier).astype(jnp.int32), axis=1)
    slot = owner * cap + rank
    place = owner * LANES + rank
    wanted = jnp.sum(
        jnp.where(
            place[None, None, :]
            == (jnp.arange(n)[:, None] * LANES + jnp.arange(LANES)[None, :])[:, :, None],
            code[None, None, :],
            0,
        ),
        axis=2,
    ).reshape(n, 1, LANES)

    half = lax.axis_size("mp")
    units = (g_count // half) * (width // LANES) * (BS // 16)
    per = -(-units // n)
    part_rows = pairs * g_count * BS
    rows_per = -(-part_rows // n // 16) * 16
    parts = part_rows // rows_per
    bf = jnp.bfloat16
    own = blocks * heads
    dma = pltpu.SemaphoreType.DMA
    att = pl.pallas_call(
        functools.partial(attend_kernel, n, cap, heads, blocks, g_count),
        out_shape=jax.ShapeDtypeStruct((pairs, tokens, LANES), bf),
        in_specs=[pl.BlockSpec(memory_space=pltpu.HBM)] * 2
        + vmem_specs(1)
        + [pl.BlockSpec(memory_space=pltpu.SMEM)] * 2,
        out_specs=pl.BlockSpec(memory_space=pltpu.VMEM),
        scratch_shapes=[
            pltpu.VMEM((tokens, width), bf),
            pltpu.VMEM(qkv_weight.shape, bf),
            pltpu.VMEM((n, 1, LANES), jnp.int32),
            pltpu.SMEM((n, 1, LANES), jnp.int32),
            pltpu.VMEM((units, 16, LANES), bf),
            pltpu.VMEM((n, per, 16, LANES), bf),
            pltpu.VMEM((per, 16, LANES), bf),
            pltpu.VMEM((half, units, 16, LANES), bf),
            pltpu.VMEM((g_count * BS, width), bf),
            pltpu.VMEM((own, BS, LANES), bf),
            pltpu.VMEM((own, BS, LANES), bf),
            pltpu.VMEM((n * cap, BS, LANES), bf),
            pltpu.VMEM((n * cap, BS, LANES), bf),
            pltpu.VMEM((heads, BS, LANES), bf),
            pltpu.VMEM((heads, BS, LANES), bf),
            pltpu.VMEM((own + 2 * heads, BS, LANES), bf),
            pltpu.VMEM((heads, g_count * BS, LANES), bf),
            pltpu.VMEM((heads, g_count * BS, LANES), bf),
            pltpu.VMEM((parts, 2, rows_per, LANES), bf),
            pltpu.VMEM((n, 2, rows_per, LANES), bf),
            pltpu.VMEM((rows_per, LANES), bf),
            pltpu.VMEM((parts, rows_per, LANES), bf),
            pltpu.VMEM((own, BS, (3 + g_count) * BS), jnp.float32),
        ]
        + [dma((n,))] * 8
        + [dma((2,))] * 2
        + [dma((n,))] * 4
        + [dma((half,))] * 2
        + [dma(()), dma((4,))],
        cost_estimate=pl.CostEstimate(
            flops=30_000_000_000, bytes_accessed=20_000_000, transcendentals=0
        ),
        compiler_params=pltpu.CompilerParams(
            collective_id=0, has_side_effects=True, vmem_limit_bytes=32 * 1024 * 1024
        ),
    )(
        pltpu.with_memory_space_constraint(states, pltpu.HBM),
        pltpu.with_memory_space_constraint(qkv_weight, pltpu.HBM),
        wanted,
        slot,
        global_ids,
    )

    chunks = 4
    rows = tokens // chunks
    link = jnp.bfloat16
    return pl.pallas_call(
        functools.partial(tail_kernel, chunks),
        out_shape=jax.ShapeDtypeStruct((tokens, width), bf),
        in_specs=vmem_specs(7),
        out_specs=pl.BlockSpec(memory_space=pltpu.VMEM),
        scratch_shapes=[pltpu.VMEM((chunks, rows, width), link)] * 4
        + [dma((chunks,))] * 4
        + [pltpu.VMEM((chunks, rows, width), bf)],
        compiler_params=pltpu.CompilerParams(
            collective_id=1, has_side_effects=True, vmem_limit_bytes=32 * 1024 * 1024
        ),
    )(
        att,
        states,
        out_weight,
        up_weight,
        down_weight,
        attn_gain.reshape(1, width),
        mlp_gain.reshape(1, width),
    )


def solution(mesh):
    in_specs = (
        P("seq", None),
        P(None, None, "mp"),
        P("mp", None),
        P(None, "mp"),
        P("mp", None),
        P(),
        P(),
        P(),
        P("mp", "seq", None, None),
        P("mp", "seq", None, None),
    )
    out_specs = P("seq", None)
    return jax.shard_map(shards, mesh=mesh, in_specs=in_specs, out_specs=out_specs, check_vma=False)
```

```python
import functools

import jax
import jax.numpy as jnp
from jax import lax
from jax.experimental import pallas as pl
from jax.experimental.pallas import tpu as pltpu
from jax.sharding import PartitionSpec as P

HD = 64
BS = 64
R = 3
LANES = 128
MESH = pl.DeviceIdType.MESH

EPSILON = 1e-05
NEGATIVE = -1e30


def layer_norm(inputs, scales):
    center = jnp.mean(inputs, axis=-1, keepdims=True)
    shifted = inputs - center
    spread = jnp.mean(shifted * shifted, axis=-1, keepdims=True)
    return shifted * lax.rsqrt(spread + EPSILON) * scales


def dot_t(a, b):
    return lax.dot_general(a, b, (((1,), (1,)), ((), ())), preferred_element_type=jnp.float32)


def dot(a, b):
    return jnp.dot(a, b, preferred_element_type=jnp.float32)


def swap_halves(x):
    return pltpu.roll(x, HD, 1)


def attend_kernel(
    n,
    cap,
    heads,
    blocks,
    g_count,
    states_hbm,
    weight_hbm,
    wanted,
    slot,
    gids,
    att,
    states,
    weight,
    tab,
    tab_s,
    cand,
    cand_in,
    pick,
    gath,
    gstates,
    kvb,
    qpad,
    stage,
    rr,
    halo_l,
    halo_r,
    win,
    gq,
    gkv,
    part,
    part_in,
    gmine,
    gout,
    scores,
    s_tab,
    r_tab,
    s_cand,
    r_cand,
    s_gath,
    r_gath,
    s_rand,
    r_rand,
    s_halo,
    r_halo,
    s_part,
    r_part,
    s_gout,
    r_gout,
    s_mp,
    r_mp,
    l_sem,
    w_sem,
):
    me = lax.axis_index("seq")
    mine = lax.axis_index("mp")
    pairs = heads // 2
    width = states.shape[1]
    cols = width // LANES
    quarters = BS // 16
    half = gath.shape[0]
    gper = gath.shape[1] // (cols * quarters)
    units = gper * cols * quarters
    per = cand_in.shape[1]
    cand_parts = units // per
    rows_per = part_in.shape[2]
    part_parts = part.shape[0]
    left = lax.rem(me + n - 1, n)
    right = lax.rem(me + 1, n)

    def peer(k):
        return lax.rem(me + k, n)

    def each_peer(body):
        def step(k, carry):
            body(peer(k))
            return carry

        lax.fori_loop(1, n, step, 0)

    def guarded(limit, who, body):
        if limit < n:
            pl.when(who < limit)(body)
        else:
            body()

    def remote(src, dst, ssem, rsem, d):
        return pltpu.make_async_remote_copy(
            src_ref=src,
            dst_ref=dst,
            send_sem=ssem,
            recv_sem=rsem,
            device_id={"seq": d},
            device_id_type=MESH,
        )

    def tab_copy(d, owner):
        return remote(wanted.at[d], tab.at[owner], s_tab.at[d], r_tab.at[owner], d)

    def cand_copy(d, owner, at):
        return remote(
            cand.at[pl.ds(at * per, per)], cand_in.at[owner], s_cand.at[d], r_cand.at[owner], d
        )

    def gath_copy(d, owner):
        return remote(
            pick, gath.at[mine, pl.ds(owner * per, per)], s_gath.at[d], r_gath.at[owner], d
        )

    def rand_copy(d, owner):
        return remote(
            stage.at[pl.ds(d * cap, cap)],
            rr.at[pl.ds(owner * cap, cap)],
            s_rand.at[d],
            r_rand.at[owner],
            d,
        )

    def part_copy(d, owner, at):
        return remote(part.at[at], part_in.at[owner], s_part.at[d], r_part.at[owner], d)

    def gout_copy(d, owner):
        return remote(gmine, gout.at[owner], s_gout.at[d], r_gout.at[owner], d)

    def mp_copy(k, owner):
        other = lax.rem(mine + k, half)
        return pltpu.make_async_remote_copy(
            src_ref=gath.at[mine],
            dst_ref=gath.at[owner],
            send_sem=s_mp.at[k],
            recv_sem=r_mp.at[owner],
            device_id={"mp": other},
            device_id_type=MESH,
        )

    to_right = remote(
        kvb.at[pl.ds((blocks - 1) * heads, heads)], halo_l, s_halo.at[0], r_halo.at[0], right
    )
    to_left = remote(kvb.at[pl.ds(0, heads)], halo_r, s_halo.at[1], r_halo.at[1], left)

    loads = [pltpu.make_async_copy(states_hbm, states, w_sem.at[3])] + [
        pltpu.make_async_copy(weight_hbm.at[i], weight.at[i], w_sem.at[i]) for i in (1, 2, 0)
    ]
    for load in loads:
        load.start()

    barrier = pltpu.get_barrier_semaphore()
    each_peer(
        lambda d: pl.semaphore_signal(barrier, inc=1, device_id={"seq": d}, device_id_type=MESH)
    )
    for k in range(1, half):
        pl.semaphore_signal(
            barrier, inc=1, device_id={"mp": lax.rem(mine + k, half)}, device_id_type=MESH
        )

    loads[0].wait()
    for i in range(gper):
        local = lax.rem(gids[mine * gper + i], blocks)
        for j in range(cols):
            cut = slice(j * LANES, (j + 1) * LANES)
            piece = states[0:BS, cut]
            for b in range(1, blocks):
                piece = jnp.where(local == b, states[b * BS : (b + 1) * BS, cut], piece)
            for q in range(quarters):
                cand[(i * cols + j) * quarters + q] = piece[q * 16 : (q + 1) * 16]
    tab[me] = wanted[me]

    def own_cand():
        cand_in[me] = cand[pl.ds(me * per, per)]

    guarded(cand_parts, me, own_cand)
    loads[1].wait()
    loads[2].wait()

    lane = lax.broadcasted_iota(jnp.int32, (BS, LANES), 1)
    low = lane < HD
    x = states[...]
    for j in range(pairs):
        cut = slice(j * LANES, (j + 1) * LANES)
        k = dot(x, weight[1, :, cut])
        v = dot(x, weight[2, :, cut])
        for b in range(blocks):
            kb, vb = k[b * BS : (b + 1) * BS], v[b * BS : (b + 1) * BS]
            kvb[b * heads + 2 * j] = jnp.where(low, kb, swap_halves(vb)).astype(jnp.bfloat16)
            kvb[b * heads + 2 * j + 1] = jnp.where(low, swap_halves(kb), vb).astype(jnp.bfloat16)

    pl.semaphore_wait(barrier, n - 1 + half - 1)
    each_peer(lambda d: tab_copy(d, me).start())
    each_peer(lambda d: guarded(cand_parts, d, lambda: cand_copy(d, me, d).start()))
    to_right.start()
    to_left.start()

    loads[3].wait()
    scaling = HD ** (-0.5)
    for j in range(pairs):
        cut = slice(j * LANES, (j + 1) * LANES)
        q = dot(x, weight[0, :, cut]).astype(jnp.bfloat16).astype(jnp.float32) * scaling
        for b in range(blocks):
            qb = q[b * BS : (b + 1) * BS]
            qpad[b * heads + 2 * j] = jnp.where(low, qb, 0.0).astype(jnp.bfloat16)
            qpad[b * heads + 2 * j + 1] = jnp.where(low, swap_halves(qb), 0.0).astype(jnp.bfloat16)

    def relay():
        each_peer(lambda d: cand_copy(d, d, me).wait_recv())
        for u in range(per):
            g = (me * per + u) // (cols * quarters)
            wanted_id = gids[mine * gper + g]

            def choose(d, so_far):
                here = (wanted_id >= d * blocks) & (wanted_id < (d + 1) * blocks)
                return jnp.where(here, cand_in[d, u], so_far)

            pick[u] = lax.fori_loop(1, n, choose, cand_in[0, u])
        gath[mine, pl.ds(me * per, per)] = pick[...]
        each_peer(lambda d: gath_copy(d, me).start())

    guarded(cand_parts, me, relay)

    each_peer(lambda d: tab_copy(d, d).wait_recv())
    table = pltpu.make_async_copy(tab, tab_s, l_sem)
    table.start()
    table.wait()

    def serve(d):
        for c in range(cap):
            stage[d * cap + c] = kvb[tab_s[d, 0, c]]
        rand_copy(d, me).start()

    def serve_some(start, stop):
        def step(k, carry):
            serve(peer(k))
            return carry

        lax.fori_loop(start, stop, step, 0)

    for c in range(cap):
        rr[me * cap + c] = kvb[tab_s[me, 0, c]]

    each_peer(lambda d: guarded(cand_parts, d, lambda: gath_copy(d, d).wait_recv()))
    for k in range(1, half):
        mp_copy(k, mine).start()
    for k in range(1, half):
        mp_copy(k, lax.rem(mine + k, half)).wait_recv()
    for g in range(g_count):
        for j in range(cols):
            for q in range(quarters):
                gstates[g * BS + q * 16 : g * BS + (q + 1) * 16, j * LANES : (j + 1) * LANES] = (
                    gath[g // gper, ((g % gper) * cols + j) * quarters + q]
                )
    gx = gstates[...]
    rows = g_count * BS
    glane = lax.broadcasted_iota(jnp.int32, (rows, LANES), 1)
    glow = glane < HD
    for j in range(pairs):
        cut = slice(j * LANES, (j + 1) * LANES)
        q = dot(gx, weight[0, :, cut]).astype(jnp.bfloat16).astype(jnp.float32) * scaling
        k = dot(gx, weight[1, :, cut])
        v = dot(gx, weight[2, :, cut])
        gq[2 * j] = jnp.where(glow, q, 0.0).astype(jnp.bfloat16)
        gq[2 * j + 1] = jnp.where(glow, swap_halves(q), 0.0).astype(jnp.bfloat16)
        gkv[2 * j] = jnp.where(glow, k, swap_halves(v)).astype(jnp.bfloat16)
        gkv[2 * j + 1] = jnp.where(glow, swap_halves(k), v).astype(jnp.bfloat16)

    for h in range(heads):
        keys = jnp.concatenate([kvb[b * heads + h] for b in range(blocks)], axis=0)
        s = dot_t(gq[h], keys)
        high = jnp.max(s, axis=-1, keepdims=True)
        e = jnp.exp(s - high)
        total = jnp.sum(e, axis=-1, keepdims=True)
        e_high = e.astype(jnp.bfloat16)
        e_low = (e - e_high.astype(jnp.float32)).astype(jnp.bfloat16)
        acc = (dot(e_high, keys) + dot(e_low, keys)) * (1.0 / total)
        level = high + jnp.log(total)
        first = level.astype(jnp.bfloat16).astype(jnp.float32)
        second = (level - first).astype(jnp.bfloat16).astype(jnp.float32)
        third = level - first - second
        packed = jnp.where(
            glane < 16,
            first,
            jnp.where(glane < 32, second, jnp.where(glow, third, acc)),
        ).astype(jnp.bfloat16)
        cuts = rows // rows_per
        for c in range(cuts):
            part[(h // 2) * cuts + c, h % 2] = packed[c * rows_per : (c + 1) * rows_per]
    each_peer(lambda d: guarded(part_parts, d, lambda: part_copy(d, me, d).start()))
    serve_some(1, n)

    to_right.wait_recv()
    to_left.wait_recv()
    win[0:heads] = halo_l[...]
    win[heads : heads + blocks * heads] = kvb[...]
    win[heads + blocks * heads :] = halo_r[...]

    near = 3 + g_count
    slot_lane = lax.broadcasted_iota(jnp.int32, (BS, near * BS), 1)

    def near_keys(at, h):
        return jnp.concatenate([win[at + t * heads] for t in range(3)] + [gkv[h]], axis=0)

    def near_step(b, carry):
        first = me * blocks + b
        start = jnp.where(first == 0, BS, 0)
        stop = jnp.where(first == n * blocks - 1, 2 * BS, 3 * BS)
        outside = (slot_lane < start) | ((slot_lane >= stop) & (slot_lane < 3 * BS))
        for h in range(heads):
            at = b * heads + h
            scores[at] = jnp.where(outside, NEGATIVE, dot_t(qpad[at], near_keys(at, h)))
        return carry

    lax.fori_loop(0, blocks, near_step, 0)

    def combine():
        part_in[me] = part[me]
        each_peer(lambda d: part_copy(d, d, me).wait_recv())
        outs = []
        for parity in range(2):

            def level(d):
                piece = part_in[d, parity].astype(jnp.float32)
                return piece, piece[:, 0:1] + piece[:, 16:17] + piece[:, 32:33]

            def top(d, best):
                return jnp.maximum(best, level(d)[1])

            best = lax.fori_loop(1, n, top, level(0)[1])

            def add(d, so_far):
                piece, high = level(d)
                factor = jnp.exp(high - best)
                return so_far[0] + piece * factor, so_far[1] + factor

            zero = (jnp.zeros((rows_per, LANES), jnp.float32), jnp.zeros((rows_per, 1), jnp.float32))
            summed, total = lax.fori_loop(0, n, add, zero)
            outs.append(summed / total)
        plow = lax.broadcasted_iota(jnp.int32, (rows_per, LANES), 1) < HD
        done = jnp.where(plow, swap_halves(outs[0]), outs[1]).astype(jnp.bfloat16)
        gmine[...] = done
        gout[me] = done
        each_peer(lambda d: gout_copy(d, me).start())

    guarded(part_parts, me, combine)

    each_peer(lambda d: rand_copy(d, d).wait_recv())

    def block_step(b, carry):
        for j in range(pairs):
            halves = []
            for h in (2 * j, 2 * j + 1):
                at = b * heads + h
                early_keys = near_keys(at, h)
                keys = jnp.concatenate([rr[slot[at * R + r]] for r in range(R)], axis=0)
                s = dot_t(qpad[at], keys)
                early_s = scores[at]
                high = jnp.maximum(
                    jnp.max(s, axis=-1, keepdims=True), jnp.max(early_s, axis=-1, keepdims=True)
                )
                e = jnp.exp(s - high)
                early_e = jnp.exp(early_s - high)
                total = jnp.sum(e, axis=-1, keepdims=True) + jnp.sum(
                    early_e, axis=-1, keepdims=True
                )
                share = 1.0 / total
                w = (e * share).astype(jnp.bfloat16)
                early_w = (early_e * share).astype(jnp.bfloat16)
                halves.append(dot(w, keys) + dot(early_w, early_keys))
            att[j, pl.ds(pl.multiple_of(b * BS, BS), BS), :] = jnp.where(
                low, swap_halves(halves[0]), halves[1]
            ).astype(jnp.bfloat16)
        return carry

    lax.fori_loop(0, blocks, block_step, 0)

    each_peer(lambda d: guarded(part_parts, d, lambda: gout_copy(d, d).wait_recv()))
    for j in range(pairs):
        for g in range(g_count):
            cuts = BS // rows_per
            at = (j * g_count + g) * cuts
            row = jnp.concatenate([gout[at + c] for c in range(cuts)], axis=0).astype(jnp.float32)
            for b in range(blocks):
                here = gids[g] == me * blocks + b
                old = att[j, b * BS : (b + 1) * BS, :].astype(jnp.float32)
                att[j, b * BS : (b + 1) * BS, :] = jnp.where(here, row, old).astype(jnp.bfloat16)

    def drain(d):
        tab_copy(d, me).wait_send()
        guarded(cand_parts, d, lambda: cand_copy(d, me, d).wait_send())
        guarded(cand_parts, me, lambda: gath_copy(d, me).wait_send())
        rand_copy(d, me).wait_send()
        guarded(part_parts, d, lambda: part_copy(d, me, d).wait_send())
        guarded(part_parts, me, lambda: gout_copy(d, me).wait_send())

    each_peer(drain)
    for k in range(1, half):
        mp_copy(k, mine).wait_send()
    to_right.wait_send()
    to_left.wait_send()


def tail_kernel(
    chunks,
    att,
    states,
    out_w,
    up_w,
    down_w,
    gain1,
    gain2,
    out,
    mine1,
    theirs1,
    mine2,
    theirs2,
    s1,
    r1,
    s2,
    r2,
    normed,
):
    other = 1 - lax.axis_index("mp")
    barrier = pltpu.get_barrier_semaphore()
    pl.semaphore_signal(barrier, inc=1, device_id={"mp": other}, device_id_type=MESH)
    pl.semaphore_wait(barrier, 1)
    rows = states.shape[0] // chunks

    def swap(mine, theirs, ssem, rsem, c):
        return pltpu.make_async_remote_copy(
            src_ref=mine.at[c],
            dst_ref=theirs.at[c],
            send_sem=ssem.at[c],
            recv_sem=rsem.at[c],
            device_id={"mp": other},
            device_id_type=MESH,
        )

    for c in range(chunks):
        cut = slice(c * rows, (c + 1) * rows)
        acc = dot(att[0, cut, :], out_w[0:LANES, :])
        for j in range(1, att.shape[0]):
            acc = acc + dot(att[j, cut, :], out_w[j * LANES : (j + 1) * LANES, :])
        mine1[c] = acc.astype(mine1.dtype)
        swap(mine1, theirs1, s1, r1, c).start()
    for c in range(chunks):
        cut = slice(c * rows, (c + 1) * rows)
        swap(mine1, theirs1, s1, r1, c).wait_recv()
        summed = mine1[c].astype(jnp.float32) + theirs1[c].astype(jnp.float32)
        norm = layer_norm(states[cut, :].astype(jnp.float32) + summed, gain1[...])
        norm = norm.astype(jnp.bfloat16)
        normed[c] = norm
        v = dot(norm, up_w[...])
        hidden = (v * (1.0 + lax.erf(v * (0.5**0.5))) * 0.5).astype(jnp.bfloat16)
        mine2[c] = dot(hidden, down_w[...]).astype(mine2.dtype)
        swap(mine2, theirs2, s2, r2, c).start()
    for c in range(chunks):
        cut = slice(c * rows, (c + 1) * rows)
        swap(mine2, theirs2, s2, r2, c).wait_recv()
        summed = mine2[c].astype(jnp.float32) + theirs2[c].astype(jnp.float32)
        out[cut, :] = layer_norm(normed[c].astype(jnp.float32) + summed, gain2[...]).astype(
            jnp.bfloat16
        )
    for c in range(chunks):
        swap(mine1, theirs1, s1, r1, c).wait_send()
        swap(mine2, theirs2, s2, r2, c).wait_send()


def vmem_specs(count):
    return [pl.BlockSpec(memory_space=pltpu.VMEM)] * count


def shards(
    states,
    qkv_weight,
    out_weight,
    up_weight,
    down_weight,
    attn_gain,
    mlp_gain,
    global_ids,
    random_owner,
    random_local,
):
    tokens, width = states.shape
    heads = qkv_weight.shape[2] // HD
    pairs = heads // 2
    blocks = tokens // BS
    g_count = global_ids.shape[0]
    n = lax.axis_size("seq")

    owner = random_owner.reshape(-1)
    items = owner.shape[0]
    cap = max(2, items // n + 1)
    head_list = jnp.broadcast_to(
        jnp.arange(heads, dtype=jnp.int32)[None, :, None], (blocks, heads, R)
    ).reshape(-1)
    code = random_local.reshape(-1) * heads + head_list
    earlier = jnp.arange(items)[:, None] > jnp.arange(items)[None, :]
    rank = jnp.sum(((owner[:, None] == owner[None, :]) & earlier).astype(jnp.int32), axis=1)
    slot = owner * cap + rank
    place = owner * LANES + rank
    wanted = jnp.sum(
        jnp.where(
            place[None, None, :]
            == (jnp.arange(n)[:, None] * LANES + jnp.arange(LANES)[None, :])[:, :, None],
            code[None, None, :],
            0,
        ),
        axis=2,
    ).reshape(n, 1, LANES)

    half = lax.axis_size("mp")
    units = (g_count // half) * (width // LANES) * (BS // 16)
    per = -(-units // n)
    part_rows = pairs * g_count * BS
    rows_per = -(-part_rows // n // 16) * 16
    parts = part_rows // rows_per
    bf = jnp.bfloat16
    own = blocks * heads
    dma = pltpu.SemaphoreType.DMA
    att = pl.pallas_call(
        functools.partial(attend_kernel, n, cap, heads, blocks, g_count),
        out_shape=jax.ShapeDtypeStruct((pairs, tokens, LANES), bf),
        in_specs=[pl.BlockSpec(memory_space=pltpu.HBM)] * 2
        + vmem_specs(1)
        + [pl.BlockSpec(memory_space=pltpu.SMEM)] * 2,
        out_specs=pl.BlockSpec(memory_space=pltpu.VMEM),
        scratch_shapes=[
            pltpu.VMEM((tokens, width), bf),
            pltpu.VMEM(qkv_weight.shape, bf),
            pltpu.VMEM((n, 1, LANES), jnp.int32),
            pltpu.SMEM((n, 1, LANES), jnp.int32),
            pltpu.VMEM((units, 16, LANES), bf),
            pltpu.VMEM((n, per, 16, LANES), bf),
            pltpu.VMEM((per, 16, LANES), bf),
            pltpu.VMEM((half, units, 16, LANES), bf),
            pltpu.VMEM((g_count * BS, width), bf),
            pltpu.VMEM((own, BS, LANES), bf),
            pltpu.VMEM((own, BS, LANES), bf),
            pltpu.VMEM((n * cap, BS, LANES), bf),
            pltpu.VMEM((n * cap, BS, LANES), bf),
            pltpu.VMEM((heads, BS, LANES), bf),
            pltpu.VMEM((heads, BS, LANES), bf),
            pltpu.VMEM((own + 2 * heads, BS, LANES), bf),
            pltpu.VMEM((heads, g_count * BS, LANES), bf),
            pltpu.VMEM((heads, g_count * BS, LANES), bf),
            pltpu.VMEM((parts, 2, rows_per, LANES), bf),
            pltpu.VMEM((n, 2, rows_per, LANES), bf),
            pltpu.VMEM((rows_per, LANES), bf),
            pltpu.VMEM((parts, rows_per, LANES), bf),
            pltpu.VMEM((own, BS, (3 + g_count) * BS), jnp.float32),
        ]
        + [dma((n,))] * 8
        + [dma((2,))] * 2
        + [dma((n,))] * 4
        + [dma((half,))] * 2
        + [dma(()), dma((4,))],
        cost_estimate=pl.CostEstimate(
            flops=30_000_000_000, bytes_accessed=20_000_000, transcendentals=0
        ),
        compiler_params=pltpu.CompilerParams(
            collective_id=0, has_side_effects=True, vmem_limit_bytes=32 * 1024 * 1024
        ),
    )(
        pltpu.with_memory_space_constraint(states, pltpu.HBM),
        pltpu.with_memory_space_constraint(qkv_weight, pltpu.HBM),
        wanted,
        slot,
        global_ids,
    )

    chunks = 4
    rows = tokens // chunks
    link = jnp.bfloat16
    return pl.pallas_call(
        functools.partial(tail_kernel, chunks),
        out_shape=jax.ShapeDtypeStruct((tokens, width), bf),
        in_specs=vmem_specs(7),
        out_specs=pl.BlockSpec(memory_space=pltpu.VMEM),
        scratch_shapes=[pltpu.VMEM((chunks, rows, width), link)] * 4
        + [dma((chunks,))] * 4
        + [pltpu.VMEM((chunks, rows, width), bf)],
        compiler_params=pltpu.CompilerParams(
            collective_id=1, has_side_effects=True, vmem_limit_bytes=32 * 1024 * 1024
        ),
    )(
        att,
        states,
        out_weight,
        up_weight,
        down_weight,
        attn_gain.reshape(1, width),
        mlp_gain.reshape(1, width),
    )


def solution(mesh):
    in_specs = (
        P("seq", None),
        P(None, None, "mp"),
        P("mp", None),
        P(None, "mp"),
        P("mp", None),
        P(),
        P(),
        P(),
        P("mp", "seq", None, None),
        P("mp", "seq", None, None),
    )
    out_specs = P("seq", None)
    return jax.shard_map(shards, mesh=mesh, in_specs=in_specs, out_specs=out_specs, check_vma=False)
```
